8 devices in a mesh: dp: 1 (over z), tp: 2 (over y), cp: 4 (over x, core).
Axes of the slice: x: 2, y: 2, z: 1, core: 2. Of those that a mesh axis runs over, the one named last changes fastest.
Arguments:
- x_in: bfloat16 [4096, 2048], P(('dp', 'cp', 'tp'))
- w_query: bfloat16 [2048, 32, 64], P(None, 'tp')
- w_key: bfloat16 [2048, 8, 64], P(None, 'tp')
- w_value: bfloat16 [2048, 8, 64], P(None, 'tp')
- w_out: bfloat16 [32, 64, 2048], P('tp')
- d_out: bfloat16 [4096, 2048], P(('dp', 'cp', 'tp'))
Outputs:
- output 1: bfloat16 [4096, 2048], P(('dp', 'cp', 'tp'))
- output 2: bfloat16 [4096, 2048], P(('dp', 'cp', 'tp'))
- output 3: bfloat16 [4, 2048, 32, 64], P(('dp', 'cp'), None, 'tp')
- output 4: bfloat16 [4, 2048, 8, 64], P(('dp', 'cp'), None, 'tp')
- output 5: bfloat16 [4, 2048, 8, 64], P(('dp', 'cp'), None, 'tp')
- output 6: bfloat16 [4, 32, 64, 2048], P(('dp', 'cp'), 'tp')
All inputs are finite; a program needn't handle non-finite values.
Results may differ from the reference program's by a relative error of at most 0.0112094.
Values are sent between devices in bfloat16 or wider.
A program may use at most 1 GiB of HBM per device.

```python
import math
import jax
import jax.numpy as jnp
from jax import lax

MODEL_DIM = 2048
NUM_HEADS = 32
NUM_KV_HEADS = 8
HEAD_DIM = 64
SEQ_LEN = 4096
SEQ_SHARDS = 4
QUERY_BLOCK = 32


def setup_inputs(seed: int = 0, part: int = 0) -> dict:
    shared_keys = jax.random.split(jax.random.key(seed), 4)
    part_keys = jax.random.split(jax.random.fold_in(jax.random.key(seed), part), 2)
    logit_gain = 1.6
    in_scale = 1.0 / math.sqrt(MODEL_DIM)
    x_in = jax.random.normal(part_keys[0], (SEQ_LEN, MODEL_DIM), jnp.float32)
    w_query = jax.random.normal(shared_keys[0], (MODEL_DIM, NUM_HEADS, HEAD_DIM), jnp.float32) * (logit_gain * in_scale)
    w_key = jax.random.normal(shared_keys[1], (MODEL_DIM, NUM_KV_HEADS, HEAD_DIM), jnp.float32) * (logit_gain * in_scale)
    w_value = jax.random.normal(shared_keys[2], (MODEL_DIM, NUM_KV_HEADS, HEAD_DIM), jnp.float32) * in_scale
    w_out = jax.random.normal(shared_keys[3], (NUM_HEADS, HEAD_DIM, MODEL_DIM), jnp.float32) / math.sqrt(NUM_HEADS * HEAD_DIM)
    d_out = jax.random.normal(part_keys[1], (SEQ_LEN, MODEL_DIM), jnp.float32)
    return {"x_in": x_in.astype(jnp.bfloat16), "w_query": w_query.astype(jnp.bfloat16), "w_key": w_key.astype(jnp.bfloat16), "w_value": w_value.astype(jnp.bfloat16), "w_out": w_out.astype(jnp.bfloat16), "d_out": d_out.astype(jnp.bfloat16)}


def stored_positions():
    half_rows = SEQ_LEN // (2 * SEQ_SHARDS)
    row_ids = jnp.arange(SEQ_LEN, dtype=jnp.int32)
    shard_id = row_ids // (2 * half_rows)
    within = row_ids % (2 * half_rows)
    return jnp.where(within < half_rows, shard_id * half_rows + within, (2 * SEQ_SHARDS - 1 - shard_id) * half_rows + within - half_rows)


def reference(x_in, w_query, w_key, w_value, w_out, d_out):
    groups = NUM_HEADS // NUM_KV_HEADS
    attn_scale = 1.0 / math.sqrt(HEAD_DIM)
    n_blocks = SEQ_LEN // QUERY_BLOCK
    shard_rows = SEQ_LEN // SEQ_SHARDS
    q_cols = NUM_HEADS * HEAD_DIM
    kv_cols = NUM_KV_HEADS * HEAD_DIM
    wq_flat = w_query.reshape(MODEL_DIM, q_cols)
    wk_flat = w_key.reshape(MODEL_DIM, kv_cols)
    wv_flat = w_value.reshape(MODEL_DIM, kv_cols)
    wo_flat = w_out.reshape(q_cols, MODEL_DIM)
    q_flat = jnp.dot(x_in, wq_flat, preferred_element_type=jnp.float32).astype(jnp.bfloat16)
    k_flat = jnp.dot(x_in, wk_flat, preferred_element_type=jnp.float32).astype(jnp.bfloat16)
    v_flat = jnp.dot(x_in, wv_flat, preferred_element_type=jnp.float32).astype(jnp.bfloat16)
    positions = stored_positions()
    k_heads = k_flat.reshape(SEQ_LEN, NUM_KV_HEADS, HEAD_DIM).astype(jnp.float32)
    v_heads = v_flat.reshape(SEQ_LEN, NUM_KV_HEADS, HEAD_DIM).astype(jnp.float32)
    q_blocks = q_flat.reshape(n_blocks, QUERY_BLOCK, NUM_KV_HEADS, groups, HEAD_DIM)
    pos_blocks = positions.reshape(n_blocks, QUERY_BLOCK)

    def block_scores(q_blk, pos_blk):
        scores = jnp.einsum("qhgd,khd->qhgk", q_blk.astype(jnp.float32), k_heads) * attn_scale
        visible = pos_blk[:, None, None, None] >= positions[None, None, None, :]
        return jnp.where(visible, scores, -jnp.inf)

    def forward_block(block_in):
        q_blk, pos_blk = block_in
        scores = block_scores(q_blk, pos_blk)
        row_max = jnp.max(scores, axis=-1)
        prob_mat = jnp.exp(scores - row_max[..., None])
        row_sum = jnp.sum(prob_mat, axis=-1)
        pv_sum = jnp.einsum("qhgk,khd->qhgd", prob_mat.astype(jnp.bfloat16).astype(jnp.float32), v_heads)
        out_blk = (pv_sum / row_sum[..., None]).astype(jnp.bfloat16)
        return out_blk, row_max + jnp.log(row_sum)

    o_blocks, lse_blocks = lax.map(forward_block, (q_blocks, pos_blocks))
    o_flat = o_blocks.reshape(SEQ_LEN, q_cols)
    y_out = jnp.dot(o_flat, wo_flat, preferred_element_type=jnp.float32).astype(jnp.bfloat16)

    do_flat = jnp.dot(d_out, wo_flat.T, preferred_element_type=jnp.float32).astype(jnp.bfloat16)
    do_blocks = do_flat.reshape(n_blocks, QUERY_BLOCK, NUM_KV_HEADS, groups, HEAD_DIM)
    dot_blocks = jnp.sum(do_blocks.astype(jnp.float32) * o_blocks.astype(jnp.float32), axis=-1)

    def backward_block(grad_carry, block_in):
        dk_acc, dv_acc = grad_carry
        q_blk, pos_blk, lse_blk, do_blk, dot_blk = block_in
        scores = block_scores(q_blk, pos_blk)
        prob_mat = jnp.exp(scores - lse_blk[..., None])
        do_wide = do_blk.astype(jnp.float32)
        d_probs = jnp.einsum("qhgd,khd->qhgk", do_wide, v_heads)
        d_scores = (prob_mat * (d_probs - dot_blk[..., None])).astype(jnp.bfloat16).astype(jnp.float32)
        dv_acc = dv_acc + jnp.einsum("qhgk,qhgd->khd", prob_mat.astype(jnp.bfloat16).astype(jnp.float32), do_wide)
        dk_acc = dk_acc + jnp.einsum("qhgk,qhgd->khd", d_scores, q_blk.astype(jnp.float32)) * attn_scale
        dq_blk = jnp.einsum("qhgk,khd->qhgd", d_scores, k_heads) * attn_scale
        return (dk_acc, dv_acc), dq_blk.astype(jnp.bfloat16)

    zero_kv = jnp.zeros((SEQ_LEN, NUM_KV_HEADS, HEAD_DIM), jnp.float32)
    grad_kv, dq_blocks = lax.scan(backward_block, (zero_kv, zero_kv), (q_blocks, pos_blocks, lse_blocks, do_blocks, dot_blocks))
    dq_flat = dq_blocks.reshape(SEQ_LEN, q_cols)
    dk_flat = grad_kv[0].astype(jnp.bfloat16).reshape(SEQ_LEN, kv_cols)
    dv_flat = grad_kv[1].astype(jnp.bfloat16).reshape(SEQ_LEN, kv_cols)
    dx_sum = (jnp.dot(dq_flat, wq_flat.T, preferred_element_type=jnp.float32)
              + jnp.dot(dk_flat, wk_flat.T, preferred_element_type=jnp.float32)
              + jnp.dot(dv_flat, wv_flat.T, preferred_element_type=jnp.float32))
    grad_x = dx_sum.astype(jnp.bfloat16)
    x_shards = x_in.reshape(SEQ_SHARDS, shard_rows, MODEL_DIM).astype(jnp.float32)
    grad_wq = jnp.einsum("rsm,rsc->rmc", x_shards, dq_flat.reshape(SEQ_SHARDS, shard_rows, q_cols).astype(jnp.float32)).astype(jnp.bfloat16).reshape(SEQ_SHARDS, MODEL_DIM, NUM_HEADS, HEAD_DIM)
    grad_wk = jnp.einsum("rsm,rsc->rmc", x_shards, dk_flat.reshape(SEQ_SHARDS, shard_rows, kv_cols).astype(jnp.float32)).astype(jnp.bfloat16).reshape(SEQ_SHARDS, MODEL_DIM, NUM_KV_HEADS, HEAD_DIM)
    grad_wv = jnp.einsum("rsm,rsc->rmc", x_shards, dv_flat.reshape(SEQ_SHARDS, shard_rows, kv_cols).astype(jnp.float32)).astype(jnp.bfloat16).reshape(SEQ_SHARDS, MODEL_DIM, NUM_KV_HEADS, HEAD_DIM)
    grad_wo = jnp.einsum("rsc,rsm->rcm", o_flat.reshape(SEQ_SHARDS, shard_rows, q_cols).astype(jnp.float32), d_out.reshape(SEQ_SHARDS, shard_rows, MODEL_DIM).astype(jnp.float32)).astype(jnp.bfloat16).reshape(SEQ_SHARDS, NUM_HEADS, HEAD_DIM, MODEL_DIM)
    return y_out, grad_x, grad_wq, grad_wk, grad_wv, grad_wo
```

```python
import jax
import jax.numpy as jnp
from jax import lax
from jax.experimental import pallas as pl
from jax.experimental.pallas import tpu as pltpu
from jax.sharding import PartitionSpec as P

ROW_SPEC = P(("dp", "cp", "tp"), None)
HEAD_SPEC = P(None, "tp", None)
OUT_W_SPEC = P("tp", None, None)
GRAD_SPEC = P(("dp", "cp"), None, "tp", None)
GRAD_OUT_SPEC = P(("dp", "cp"), "tp", None, None)
NT = (((1,), (1,)), ((), ()))
TN = (((0,), (0,)), ((), ()))
F32 = jnp.float32
BF16 = jnp.bfloat16
VMEM_LIMIT = 60 * 1024 * 1024


def stored_block(pos_blk, n_blk):
    half = n_blk // 2
    return jnp.where(pos_blk < half, 2 * pos_blk, 2 * n_blk - 1 - 2 * pos_blk)


def fwd_kernel(n_blk, blk, groups, dim, q_ref, kv_ref, o_ref, lse_ref, kvt_s, rq_s, acc_s, m_s, l_s):
    step = pl.program_id(0)

    @pl.when(step == 0)
    def _():
        for b in range(n_blk):
            kvt_s[:, b * blk:(b + 1) * blk] = kv_ref[b * blk:(b + 1) * blk, :].T
        rq_s[...] = jnp.zeros_like(rq_s)

    q_t = q_ref[...].T
    for h in range(groups):
        rq_s[h, :dim, :] = q_t[h * dim:(h + 1) * dim, :]

    def tile(j, diag):
        off = pl.multiple_of(stored_block(j, n_blk) * blk, blk)
        kv_j = kv_ref[pl.ds(off, blk), :]
        v_t = kvt_s[dim:, pl.ds(off, blk)]
        for h in range(groups):
            s = jnp.dot(kv_j, rq_s[h], preferred_element_type=F32)
            if diag:
                keep = lax.broadcasted_iota(jnp.int32, s.shape, 0) <= lax.broadcasted_iota(jnp.int32, s.shape, 1)
                s = jnp.where(keep, s, -jnp.inf)
                m_new = jnp.max(s, axis=0, keepdims=True)
                p = jnp.exp(s - m_new)
                l_s[h] = jnp.sum(p, axis=0, keepdims=True)
                acc_s[h] = jnp.dot(v_t, p.astype(BF16), preferred_element_type=F32)
            else:
                m_old = m_s[h]
                m_new = jnp.maximum(m_old, jnp.max(s, axis=0, keepdims=True))
                p = jnp.exp(s - m_new)
                alpha = jnp.exp(m_old - m_new)
                l_s[h] = l_s[h] * alpha + jnp.sum(p, axis=0, keepdims=True)
                acc_s[h] = acc_s[h] * alpha + jnp.dot(v_t, p.astype(BF16), preferred_element_type=F32)
            m_s[h] = m_new

    tile(step, True)

    @pl.loop(0, step)
    def _(j):
        tile(j, False)

    outs = []
    for h in range(groups):
        outs.append((acc_s[h] / l_s[h]).astype(BF16))
        lse_ref[0, h:h + 1, :] = m_s[h] + jnp.log(l_s[h])
    o_ref[...] = jnp.concatenate(outs, axis=0).T


def bwd_kernel(n_blk, blk, groups, dim, q_ref, do_ref, o_ref, lse_ref, kv_ref, dq_ref, dkv_ref,
               kt_s, rq_s, rd_s, rqk_s, rdo_s, dot_s, dqt_s, dkv_s):
    step = pl.program_id(0)

    @pl.when(step == 0)
    def _():
        for b in range(n_blk):
            kt_s[:, b * blk:(b + 1) * blk] = kv_ref[b * blk:(b + 1) * blk, :].T
        rq_s[...] = jnp.zeros_like(rq_s)
        rd_s[...] = jnp.zeros_like(rd_s)
        dkv_s[...] = jnp.zeros_like(dkv_s)

    q = q_ref[...]
    do = do_ref[...]
    q_t = q.T
    do_t = do.T
    o_t = o_ref[...].T
    zero = jnp.zeros((blk, dim), BF16)
    for h in range(groups):
        rows = slice(h * dim, (h + 1) * dim)
        rq_s[h, :dim, :] = q_t[rows, :]
        rd_s[h, dim:, :] = do_t[rows, :]
        rqk_s[h] = jnp.concatenate([q[:, rows], zero], axis=1)
        rdo_s[h] = jnp.concatenate([zero, do[:, rows]], axis=1)
        dot_s[h] = jnp.sum(do_t[rows, :].astype(F32) * o_t[rows, :].astype(F32), axis=0, keepdims=True)
    dqt_s[...] = jnp.zeros_like(dqt_s)

    def tile(j, diag):
        off = pl.multiple_of(stored_block(j, n_blk) * blk, blk)
        kv_j = kv_ref[pl.ds(off, blk), :]
        k_t = kt_s[:dim, pl.ds(off, blk)]
        total = dkv_s[pl.ds(off, blk), :]
        for h in range(groups):
            s = jnp.dot(kv_j, rq_s[h], preferred_element_type=F32)
            p = jnp.exp(s - lse_ref[0, h:h + 1, :])
            if diag:
                keep = lax.broadcasted_iota(jnp.int32, s.shape, 0) <= lax.broadcasted_iota(jnp.int32, s.shape, 1)
                p = jnp.where(keep, p, 0.0)
            dp = jnp.dot(kv_j, rd_s[h], preferred_element_type=F32)
            ds = (p * (dp - dot_s[h])).astype(BF16)
            dqt_s[h] += jnp.dot(k_t, ds, preferred_element_type=F32)
            total += jnp.dot(ds, rqk_s[h], preferred_element_type=F32)
            total += jnp.dot(p.astype(BF16), rdo_s[h], preferred_element_type=F32)
        dkv_s[pl.ds(off, blk), :] = total

    tile(step, True)

    @pl.loop(0, step)
    def _(j):
        tile(j, False)

    scale = dim ** -0.5
    dq_ref[...] = jnp.concatenate([(dqt_s[h] * scale).astype(BF16) for h in range(groups)], axis=0).T

    @pl.when(step == n_blk - 1)
    def _():
        dkv_ref[...] = dkv_s[...].astype(BF16)


def row_block_spec(n_blk, blk, cols):
    return pl.BlockSpec((blk, cols), lambda i: (stored_block(i, n_blk), 0))


def attend(q, kv, n_blk, groups, dim):
    rows = q.shape[0]
    blk = rows // n_blk
    cols = groups * dim
    full = pl.BlockSpec((rows, 2 * dim), lambda i: (0, 0))
    elems = rows * rows * groups // 2
    return pl.pallas_call(
        lambda *refs: fwd_kernel(n_blk, blk, groups, dim, *refs),
        grid=(n_blk,),
        in_specs=[row_block_spec(n_blk, blk, cols), full],
        out_specs=[row_block_spec(n_blk, blk, cols), pl.BlockSpec((1, groups, blk), lambda i: (i, 0, 0))],
        out_shape=[jax.ShapeDtypeStruct((rows, cols), BF16), jax.ShapeDtypeStruct((n_blk, groups, blk), F32)],
        scratch_shapes=[
            pltpu.VMEM((2 * dim, rows), BF16),
            pltpu.VMEM((groups, 2 * dim, blk), BF16),
            pltpu.VMEM((groups, dim, blk), F32),
            pltpu.VMEM((groups, 1, blk), F32),
            pltpu.VMEM((groups, 1, blk), F32),
        ],
        compiler_params=pltpu.CompilerParams(dimension_semantics=("arbitrary",), vmem_limit_bytes=VMEM_LIMIT),
        cost_estimate=pl.CostEstimate(flops=elems * 4 * dim * 4, bytes_accessed=rows * cols * 6, transcendentals=elems),
        name="attend_fwd",
    )(q, kv)


def attend_grad(q, do, o, lse, kv, n_blk, groups, dim):
    rows = q.shape[0]
    blk = rows // n_blk
    cols = groups * dim
    full = pl.BlockSpec((rows, 2 * dim), lambda i: (0, 0))
    elems = rows * rows * groups // 2
    row_spec = row_block_spec(n_blk, blk, cols)
    return pl.pallas_call(
        lambda *refs: bwd_kernel(n_blk, blk, groups, dim, *refs),
        grid=(n_blk,),
        in_specs=[row_spec, row_spec, row_spec, pl.BlockSpec((1, groups, blk), lambda i: (i, 0, 0)), full],
        out_specs=[row_spec, full],
        out_shape=[jax.ShapeDtypeStruct((rows, cols), BF16), jax.ShapeDtypeStruct((rows, 2 * dim), BF16)],
        scratch_shapes=[
            pltpu.VMEM((2 * dim, rows), BF16),
            pltpu.VMEM((groups, 2 * dim, blk), BF16),
            pltpu.VMEM((groups, 2 * dim, blk), BF16),
            pltpu.VMEM((groups, blk, 2 * dim), BF16),
            pltpu.VMEM((groups, blk, 2 * dim), BF16),
            pltpu.VMEM((groups, 1, blk), F32),
            pltpu.VMEM((groups, dim, blk), F32),
            pltpu.VMEM((rows, 2 * dim), F32),
        ],
        compiler_params=pltpu.CompilerParams(dimension_semantics=("arbitrary",), vmem_limit_bytes=VMEM_LIMIT),
        cost_estimate=pl.CostEstimate(flops=elems * 10 * dim * 4, bytes_accessed=rows * cols * 8, transcendentals=elems),
        name="attend_bwd",
    )(q, do, o, lse, kv)


def solution(mesh):
    seq_shards = mesh.shape["cp"]

    def device_fn(x_blk, w_query, w_key, w_value, w_out, dy_blk):
        model_dim, q_heads, dim = w_query.shape
        kv_heads = w_key.shape[1]
        groups = q_heads // kv_heads
        q_cols = q_heads * dim
        n_blk = 2 * seq_shards
        scale = dim ** -0.5
        wq_t = w_query.transpose(1, 2, 0).reshape(q_cols, model_dim)
        wk_t = w_key.transpose(1, 2, 0)
        wv_t = w_value.transpose(1, 2, 0)
        wkv_t = jnp.stack([wk_t, wv_t], axis=1).reshape(2 * kv_heads * dim, model_dim)
        wo = w_out.reshape(q_cols, model_dim)

        def mm(a, b, dims):
            return lax.dot_general(a, b, dims, preferred_element_type=F32)

        def to_heads(a):
            return lax.all_to_all(a, "cp", split_axis=1, concat_axis=0, tiled=True)

        def to_rows(a):
            return lax.all_to_all(a, "cp", split_axis=0, concat_axis=1, tiled=True)

        x_rows = lax.all_gather(x_blk, "tp", axis=0, tiled=True)
        q_own = (mm(x_rows, wq_t, NT).astype(BF16) * scale).astype(BF16)
        kv_own = mm(x_rows, wkv_t, NT).astype(BF16)
        q_all = to_heads(q_own)
        kv_all = to_heads(kv_own)
        dy_rows = lax.all_gather(dy_blk, "tp", axis=0, tiled=True)
        o_all, lse = attend(q_all, kv_all, n_blk, groups, dim)
        do_own = mm(dy_rows, wo, NT).astype(BF16)
        do_all = to_heads(do_own)
        o_own = to_rows(o_all)
        y_part = mm(o_own, wo, (((1,), (0,)), ((), ())))
        y_blk = lax.psum_scatter(y_part, "tp", scatter_dimension=0, tiled=True).astype(BF16)

        dq_all, dkv_all = attend_grad(q_all, do_all, o_all, lse, kv_all, n_blk, groups, dim)
        grad_wo = mm(o_own, dy_rows, TN).astype(BF16).reshape(q_heads, dim, model_dim)
        dq_own = to_rows(dq_all)
        dkv_own = to_rows(dkv_all)
        dx_part = mm(dq_own, wq_t, (((1,), (0,)), ((), ()))) + mm(dkv_own, wkv_t, (((1,), (0,)), ((), ())))
        dx_blk = lax.psum_scatter(dx_part, "tp", scatter_dimension=0, tiled=True).astype(BF16)
        gq_t = mm(dq_own, x_rows, TN).astype(BF16).reshape(q_heads, dim, model_dim)
        gkv_t = mm(dkv_own, x_rows, TN).astype(BF16).reshape(kv_heads, 2, dim, model_dim)
        grad_wq = gq_t.transpose(2, 0, 1)
        grad_wk = gkv_t[:, 0].transpose(2, 0, 1)
        grad_wv = gkv_t[:, 1].transpose(2, 0, 1)
        return y_blk, dx_blk, grad_wq[None], grad_wk[None], grad_wv[None], grad_wo[None]

    return jax.shard_map(device_fn, mesh=mesh,
                         in_specs=(ROW_SPEC, HEAD_SPEC, HEAD_SPEC, HEAD_SPEC, OUT_W_SPEC, ROW_SPEC),
                         out_specs=(ROW_SPEC, ROW_SPEC, GRAD_SPEC, GRAD_SPEC, GRAD_SPEC, GRAD_OUT_SPEC),
                         check_vma=False)
```

```python
import jax
import jax.numpy as jnp
from jax import lax
from jax.experimental import pallas as pl
from jax.experimental.pallas import tpu as pltpu
from jax.sharding import PartitionSpec as P

ROW_SPEC = P(("dp", "cp", "tp"), None)
HEAD_SPEC = P(None, "tp", None)
OUT_W_SPEC = P("tp", None, None)
GRAD_SPEC = P(("dp", "cp"), None, "tp", None)
GRAD_OUT_SPEC = P(("dp", "cp"), "tp", None, None)
NT = (((1,), (1,)), ((), ()))
TN = (((0,), (0,)), ((), ()))
NN = (((1,), (0,)), ((), ()))
F32 = jnp.float32
BF16 = jnp.bfloat16
VMEM_LIMIT = 60 * 1024 * 1024


def half_of(pos_blk, n_blk):
    return jnp.where(pos_blk < n_blk // 2, 0, 1)


def shard_of(pos_blk, n_blk):
    return jnp.where(pos_blk < n_blk // 2, pos_blk, n_blk - 1 - pos_blk)


def stored_block(pos_blk, n_blk):
    return 2 * shard_of(pos_blk, n_blk) + half_of(pos_blk, n_blk)


def keep_mask(shape):
    return lax.broadcasted_iota(jnp.int32, shape, 0) <= lax.broadcasted_iota(jnp.int32, shape, 1)


def load_keys(n_blk, own_ref, other_ref, kv_s, kvt_s):
    own_half = lax.axis_index("tp")
    for b in range(n_blk):
        half, shard = (0, b) if b < n_blk // 2 else (1, n_blk - 1 - b)
        block = jnp.where(own_half == half, own_ref[shard], other_ref[shard])
        kv_s[b] = block
        kvt_s[b] = block.T


def load_queries(n_blk, pos, own_ref, other_ref):
    return jnp.where(lax.axis_index("tp") == half_of(pos, n_blk), own_ref[...], other_ref[...])


def fwd_kernel(n_blk, groups, dim, first, *refs):
    q_own, q_other, kv_own, kv_other = refs[:4]
    o_ref, lse_ref, kv_s, kvt_s, rq_s, acc_s, m_s, l_s = refs[-8:]
    pos = first + pl.program_id(0)

    @pl.when(pl.program_id(0) == 0)
    def _():
        load_keys(n_blk, kv_own, kv_other, kv_s, kvt_s)
        rq_s[...] = jnp.zeros_like(rq_s)

    q_t = load_queries(n_blk, pos, q_own, q_other).T
    for h in range(groups):
        rq_s[h, :dim, :] = q_t[h * dim:(h + 1) * dim, :]

    def tile(j, diag):
        kv_j = kv_s[j]
        v_t = kvt_s[j, dim:, :]
        for h in range(groups):
            s = jnp.dot(kv_j, rq_s[h], preferred_element_type=F32)
            if diag:
                s = jnp.where(keep_mask(s.shape), s, -jnp.inf)
                m_new = jnp.max(s, axis=0, keepdims=True)
                p = jnp.exp(s - m_new)
                l_s[h] = jnp.sum(p, axis=0, keepdims=True)
                acc_s[h] = jnp.dot(v_t, p.astype(BF16), preferred_element_type=F32)
            else:
                m_old = m_s[h]
                m_new = jnp.maximum(m_old, jnp.max(s, axis=0, keepdims=True))
                p = jnp.exp(s - m_new)
                alpha = jnp.exp(m_old - m_new)
                l_s[h] = l_s[h] * alpha + jnp.sum(p, axis=0, keepdims=True)
                acc_s[h] = acc_s[h] * alpha + jnp.dot(v_t, p.astype(BF16), preferred_element_type=F32)
            m_s[h] = m_new

    tile(pos, True)

    @pl.loop(0, pos)
    def _(j):
        tile(j, False)

    for h in range(groups):
        o_ref[h * dim:(h + 1) * dim, :] = (acc_s[h] / l_s[h]).astype(BF16)
        lse_ref[h:h + 1, :] = m_s[h] + jnp.log(l_s[h])


def bwd_kernel(n_blk, groups, dim, first, count, *refs):
    q_own, q_other, kv_own, kv_other, do_ref, o_ref, lse_ref = refs[:7]
    upper = first > 0
    g_ref = refs[7 if upper else 8]
    kv_s, kvt_s, rq_s, rd_s, rqk_s, rdo_s, dot_s, dqt_s, dkv_s = refs[-9:]
    step = pl.program_id(0)
    pos = first + step
    blk = do_ref.shape[0]
    cols = groups * dim

    @pl.when(step == 0)
    def _():
        load_keys(n_blk, kv_own, kv_other, kv_s, kvt_s)
        rq_s[...] = jnp.zeros_like(rq_s)
        rd_s[...] = jnp.zeros_like(rd_s)
        dkv_s[...] = jnp.zeros_like(dkv_s) if upper else refs[7][...]

    q = load_queries(n_blk, pos, q_own, q_other)
    do = do_ref[...]
    q_t = q.T
    do_t = do.T
    zero = jnp.zeros((blk, dim), BF16)
    for h in range(groups):
        rows = slice(h * dim, (h + 1) * dim)
        rq_s[h, :dim, :] = q_t[rows, :]
        rd_s[h, dim:, :] = do_t[rows, :]
        rqk_s[h] = jnp.concatenate([q[:, rows], zero], axis=1)
        rdo_s[h] = jnp.concatenate([zero, do[:, rows]], axis=1)
        dot_s[h] = jnp.sum(do_t[rows, :].astype(F32) * o_ref[rows, :].astype(F32), axis=0, keepdims=True)
    dqt_s[...] = jnp.zeros_like(dqt_s)

    def tile(j, diag):
        kv_j = kv_s[j]
        k_t = kvt_s[j, :dim, :]
        total = dkv_s[j]
        for h in range(groups):
            s = jnp.dot(kv_j, rq_s[h], preferred_element_type=F32)
            p = jnp.exp(s - lse_ref[h:h + 1, :])
            if diag:
                p = jnp.where(keep_mask(s.shape), p, 0.0)
            dp = jnp.dot(kv_j, rd_s[h], preferred_element_type=F32)
            ds = (p * (dp - dot_s[h])).astype(BF16)
            dqt_s[h] += jnp.dot(k_t, ds, preferred_element_type=F32)
            total += jnp.dot(ds, rqk_s[h], preferred_element_type=F32)
            total += jnp.dot(p.astype(BF16), rdo_s[h], preferred_element_type=F32)
        dkv_s[j] = total

    tile(pos, True)

    @pl.loop(0, pos)
    def _(j):
        tile(j, False)

    shard = shard_of(pos, n_blk)
    for h in range(groups):
        g_ref[shard, h * dim:(h + 1) * dim, :] = dqt_s[h].astype(BF16)

    @pl.when(step == count - 1)
    def _():
        for b in range(first, first + count):
            s = b if b < n_blk // 2 else n_blk - 1 - b
            g_ref[s, cols:, :] = dkv_s[b].astype(BF16).T
        if upper:
            refs[8][...] = dkv_s[:first]


def key_specs(n_half, blk, groups, dim, first):
    cols = groups * dim
    query = pl.BlockSpec((None, blk, cols), lambda i: (shard_of(first + i, 2 * n_half), 0, 0))
    keys = pl.BlockSpec((n_half, blk, 2 * dim), lambda i: (0, 0, cols // (2 * dim)))
    return [query, query, keys, keys]


def feature_spec(n_blk, cols, blk, first):
    return pl.BlockSpec((None, cols, blk), lambda i: (shard_of(first + i, n_blk), 0, half_of(first + i, n_blk)))


def attend(own, other, prev, first, count, groups, dim):
    n_half, blk = own.shape[:2]
    n_blk = 2 * n_half
    cols = groups * dim
    elems = blk * blk * groups * sum(range(first + 1, first + count + 1))
    out_shape = [jax.ShapeDtypeStruct((n_half, cols, 2 * blk), BF16), jax.ShapeDtypeStruct((n_blk, groups, blk), F32)]
    return pl.pallas_call(
        lambda *refs: fwd_kernel(n_blk, groups, dim, first, *refs),
        grid=(count,),
        in_specs=key_specs(n_half, blk, groups, dim, first) + [pl.BlockSpec(memory_space=pl.ANY)] * len(prev),
        out_specs=[feature_spec(n_blk, cols, blk, first), pl.BlockSpec((None, groups, blk), lambda i: (first + i, 0, 0))],
        out_shape=out_shape,
        input_output_aliases={4 + i: i for i in range(len(prev))},
        scratch_shapes=[
            pltpu.VMEM((n_blk, blk, 2 * dim), BF16),
            pltpu.VMEM((n_blk, 2 * dim, blk), BF16),
            pltpu.VMEM((groups, 2 * dim, blk), BF16),
            pltpu.VMEM((groups, dim, blk), F32),
            pltpu.VMEM((groups, 1, blk), F32),
            pltpu.VMEM((groups, 1, blk), F32),
        ],
        compiler_params=pltpu.CompilerParams(dimension_semantics=("arbitrary",), vmem_limit_bytes=VMEM_LIMIT),
        cost_estimate=pl.CostEstimate(flops=elems * 4 * 4 * dim, bytes_accessed=count * blk * cols * 4, transcendentals=elems),
        name="attend_fwd",
    )(own, other, own, other, *prev)


def attend_grad(own, other, do, o, lse, carried, first, count, groups, dim):
    n_half, blk = own.shape[:2]
    n_blk = 2 * n_half
    cols = groups * dim
    elems = blk * blk * groups * sum(range(first + 1, first + count + 1))
    feats = cols + 2 * dim
    keys_shape = (n_blk, blk, 2 * dim) if first else (n_half, blk, 2 * dim)
    whole = pl.BlockSpec((n_half, blk, 2 * dim), lambda i: (0, 0, 0))
    out_specs = [pl.BlockSpec((n_half, feats, blk), lambda i: (0, 0, 0))] + [whole] * (first > 0)
    out_shape = [jax.ShapeDtypeStruct((n_half, feats, blk), BF16)] + [jax.ShapeDtypeStruct((n_half, blk, 2 * dim), F32)] * (first > 0)
    return pl.pallas_call(
        lambda *refs: bwd_kernel(n_blk, groups, dim, first, count, *refs),
        grid=(count,),
        in_specs=key_specs(n_half, blk, groups, dim, first) + [
            pl.BlockSpec((None, blk, cols), lambda i: (stored_block(first + i, n_blk), 0, 0)),
            feature_spec(n_blk, cols, blk, first),
            pl.BlockSpec((None, groups, blk), lambda i: (first + i, 0, 0))] + [whole] * len(carried),
        out_specs=out_specs,
        out_shape=out_shape,
        scratch_shapes=[
            pltpu.VMEM((n_blk, blk, 2 * dim), BF16),
            pltpu.VMEM((n_blk, 2 * dim, blk), BF16),
            pltpu.VMEM((groups, 2 * dim, blk), BF16),
            pltpu.VMEM((groups, 2 * dim, blk), BF16),
            pltpu.VMEM((groups, blk, 2 * dim), BF16),
            pltpu.VMEM((groups, blk, 2 * dim), BF16),
            pltpu.VMEM((groups, 1, blk), F32),
            pltpu.VMEM((groups, dim, blk), F32),
            pltpu.VMEM(keys_shape, F32),
        ],
        compiler_params=pltpu.CompilerParams(dimension_semantics=("arbitrary",), vmem_limit_bytes=VMEM_LIMIT),
        cost_estimate=pl.CostEstimate(flops=elems * 10 * 4 * dim, bytes_accessed=count * blk * cols * 8, transcendentals=elems),
        name="attend_bwd",
    )(own, other, own, other, do, o, lse, *carried)


def solution(mesh):
    seq_shards = mesh.shape["cp"]
    swap = [(0, 1), (1, 0)]

    def device_fn(x_blk, w_query, w_key, w_value, w_out, dy_blk):
        model_dim, q_heads, dim = w_query.shape
        half_rows = x_blk.shape[0]
        kv_heads = w_key.shape[1]
        groups = q_heads // kv_heads
        cols = groups * dim
        feats = cols + 2 * dim
        q_cols = q_heads * dim
        n_half = seq_shards
        n_blk = 2 * seq_shards
        scale = dim ** -0.5
        mine = lax.axis_index("tp")
        quarter = lax.axis_index("cp")
        wo = w_out.reshape(q_cols, model_dim)
        w_all = jnp.concatenate([(w_query * scale).astype(BF16).transpose(1, 2, 0).reshape(kv_heads, cols, model_dim),
                                 w_key.transpose(1, 2, 0), w_value.transpose(1, 2, 0)], axis=1)
        w_flat = w_all.reshape(kv_heads * feats, model_dim)

        def mm(a, b, dims):
            return lax.dot_general(a, b, dims, preferred_element_type=F32)

        def exchange(a):
            return lax.ppermute(a, "tp", swap)

        def switch(a):
            return lax.all_to_all(a, "cp", split_axis=0, concat_axis=0, tiled=True)

        def project(rows):
            return mm(rows, w_flat, NT).astype(BF16).reshape(half_rows, kv_heads, feats).transpose(1, 0, 2)

        def after(value, other):
            return lax.optimization_barrier((value, other))

        def quarter_of(w):
            part = w.shape[0] // seq_shards
            return exchange(lax.dynamic_slice_in_dim(w, quarter * part, part, axis=0))

        def spread(w):
            return lax.all_gather(w, "cp", axis=0, tiled=True)

        x_peer = exchange(x_blk)
        own = switch(project(x_blk))
        x_peer, own = after(x_peer, own)
        dy_late, x_peer = after(dy_blk, x_peer)
        dy_rows = lax.all_gather(dy_late, "tp", axis=0, tiled=True)
        other = switch(project(x_peer))

        partial = attend(own, other, (), 0, n_half, groups, dim)
        dy_ready, partial = after(dy_rows, partial)
        do_own = mm(dy_ready, wo, NT).astype(BF16).reshape(2 * half_rows, kv_heads, cols).transpose(1, 0, 2)
        late, do_own = after((w_flat, wo), do_own)
        do_all = switch(do_own).reshape(n_blk, half_rows, cols)
        quarters = tuple(quarter_of(w) for w in late)
        o_all, lse = attend(own, other, partial, n_half, n_half, groups, dim)
        quarters, o_all = after(quarters, o_all)
        w_peer, wo_peer = (spread(w) for w in quarters)

        o_own = switch(o_all).reshape(q_cols, 2 * half_rows)
        g_upper, carried = attend_grad(own, other, do_all, o_all, lse, (), n_half, n_half, groups, dim)
        g_upper, o_own = after(g_upper, o_own)
        o_mine = lax.dynamic_slice_in_dim(o_own, mine * half_rows, half_rows, axis=1)
        o_peer = exchange(lax.dynamic_slice_in_dim(o_own, (1 - mine) * half_rows, half_rows, axis=1))
        g_upper = switch(g_upper)
        g_lower, = attend_grad(own, other, do_all, o_all, lse, (carried,), 0, n_half, groups, dim)
        g_lower = switch(g_lower)

        is_first = mine == 0
        g_mine = jnp.where(is_first, g_lower, g_upper)
        g_other = jnp.where(is_first, g_upper, g_lower)
        g_peer = exchange(g_other).reshape(kv_heads * feats, half_rows)

        def weight_grad(lo, hi, factor):
            def part(g, rows):
                return mm(g[:, lo:hi].reshape(kv_heads * (hi - lo), half_rows), rows, NN)

            total = part(g_mine, x_blk) + part(g_other, x_peer)
            return (total * factor).astype(BF16).reshape(1, -1, dim, model_dim).transpose(0, 3, 1, 2)

        grad_wo = mm(o_own, dy_rows, NN).astype(BF16).reshape(1, q_heads, dim, model_dim)
        y_blk = (mm(o_mine, wo, TN) + mm(o_peer, wo_peer, TN)).astype(BF16)
        grad_wq = weight_grad(0, cols, scale)
        grad_wk = weight_grad(cols, cols + dim, 1.0)
        grad_wv = weight_grad(cols + dim, feats, 1.0)
        dx_blk = (mm(g_mine.reshape(kv_heads * feats, half_rows), w_flat, TN) + mm(g_peer, w_peer, TN)).astype(BF16)
        return y_blk, dx_blk, grad_wq, grad_wk, grad_wv, grad_wo

    return jax.shard_map(device_fn, mesh=mesh,
                         in_specs=(ROW_SPEC, HEAD_SPEC, HEAD_SPEC, HEAD_SPEC, OUT_W_SPEC, ROW_SPEC),
                         out_specs=(ROW_SPEC, ROW_SPEC, GRAD_SPEC, GRAD_SPEC, GRAD_SPEC, GRAD_OUT_SPEC),
                         check_vma=False)
```

```python
import jax
import jax.numpy as jnp
from jax import lax
from jax.experimental import pallas as pl
from jax.experimental.pallas import tpu as pltpu
from jax.sharding import PartitionSpec as P

ROW_SPEC = P(("dp", "cp", "tp"), None)
HEAD_SPEC = P(None, "tp", None)
OUT_W_SPEC = P("tp", None, None)
GRAD_SPEC = P(("dp", "cp"), None, "tp", None)
GRAD_OUT_SPEC = P(("dp", "cp"), "tp", None, None)
NT = (((1,), (1,)), ((), ()))
TN = (((0,), (0,)), ((), ()))
NN = (((1,), (0,)), ((), ()))
F32 = jnp.float32
BF16 = jnp.bfloat16
VMEM_LIMIT = 60 * 1024 * 1024
FWD_SPLIT, FWD_AHEAD, FWD_BEHIND = 256, 2, 1
BWD_SPLIT, BWD_AHEAD, BWD_BEHIND = 512, 1, 0


def half_of(pos_blk, n_blk):
    return jnp.where(pos_blk < n_blk // 2, 0, 1)


def shard_of(pos_blk, n_blk):
    return jnp.where(pos_blk < n_blk // 2, pos_blk, n_blk - 1 - pos_blk)


def stored_block(pos_blk, n_blk):
    return 2 * shard_of(pos_blk, n_blk) + half_of(pos_blk, n_blk)


def keep_mask(shape, col=0):
    return lax.broadcasted_iota(jnp.int32, shape, 0) <= lax.broadcasted_iota(jnp.int32, shape, 1) + col


def load_keys(n_blk, own_ref, other_ref, kv_s, kvt_s):
    own_half = lax.axis_index("tp")
    for b in range(n_blk):
        half, shard = (0, b) if b < n_blk // 2 else (1, n_blk - 1 - b)
        block = jnp.where(own_half == half, own_ref[shard], other_ref[shard])
        kv_s[b] = block
        kvt_s[b] = block.T


def load_queries(n_blk, pos, own_ref, other_ref):
    return jnp.where(lax.axis_index("tp") == half_of(pos, n_blk), own_ref[...], other_ref[...])


def fwd_kernel(n_blk, groups, dim, first, *refs):
    q_own, q_other, kv_own, kv_other = refs[:4]
    o_ref, lse_ref, kv_s, kvt_s, rq_s, acc_s, m_s, l_s = refs[-8:]
    pos = first + pl.program_id(0)
    blk = q_own.shape[0]

    @pl.when(pl.program_id(0) == 0)
    def _():
        load_keys(n_blk, kv_own, kv_other, kv_s, kvt_s)
        rq_s[...] = jnp.zeros_like(rq_s)

    q_t = load_queries(n_blk, pos, q_own, q_other).T
    for h in range(groups):
        rq_s[h, :dim, :] = q_t[h * dim:(h + 1) * dim, :]

    def tile(j, diag):
        kv_j = kv_s[j]
        v_t = kvt_s[j, dim:, :]
        chains = [(h, slice(c, c + FWD_SPLIT)) for h in range(groups) for c in range(0, blk, FWD_SPLIT)]

        def scores(h, cs):
            return jnp.dot(kv_j, rq_s[h, :, cs], preferred_element_type=F32)

        def output(h, cs, p, alpha):
            o = jnp.dot(v_t, p, preferred_element_type=F32)
            acc_s[h, :, cs] = o if alpha is None else acc_s[h, :, cs] * alpha + o

        ahead = [scores(*chain) for chain in chains[:FWD_AHEAD]]
        behind = []
        for i, (h, cs) in enumerate(chains):
            if i + FWD_AHEAD < len(chains):
                ahead.append(scores(*chains[i + FWD_AHEAD]))
            s = ahead[i]
            if diag:
                s = jnp.where(keep_mask(s.shape, cs.start), s, -jnp.inf)
                m_new = jnp.max(s, axis=0, keepdims=True)
                p = jnp.exp(s - m_new)
                alpha = None
                l_s[h, :, cs] = jnp.sum(p, axis=0, keepdims=True)
            else:
                m_old = m_s[h, :, cs]
                m_new = jnp.maximum(m_old, jnp.max(s, axis=0, keepdims=True))
                p = jnp.exp(s - m_new)
                alpha = jnp.exp(m_old - m_new)
                l_s[h, :, cs] = l_s[h, :, cs] * alpha + jnp.sum(p, axis=0, keepdims=True)
            m_s[h, :, cs] = m_new
            behind.append((h, cs, p.astype(BF16), alpha))
            if len(behind) > FWD_BEHIND:
                output(*behind.pop(0))
        for item in behind:
            output(*item)

    tile(pos, True)

    @pl.loop(0, pos)
    def _(j):
        tile(j, False)

    for h in range(groups):
        o_ref[h * dim:(h + 1) * dim, :] = (acc_s[h] / l_s[h]).astype(BF16)
        lse_ref[h:h + 1, :] = m_s[h] + jnp.log(l_s[h])


def bwd_kernel(n_blk, groups, dim, first, count, *refs):
    q_own, q_other, kv_own, kv_other, do_ref, o_ref, lse_ref = refs[:7]
    upper = first > 0
    g_ref = refs[7 if upper else 8]
    kv_s, kvt_s, rq_s, rd_s, dot_s, dqt_s, dkv_s = refs[-7:]
    step = pl.program_id(0)
    pos = first + step
    blk = do_ref.shape[0]
    cols = groups * dim

    @pl.when(step == 0)
    def _():
        load_keys(n_blk, kv_own, kv_other, kv_s, kvt_s)
        rq_s[...] = jnp.zeros_like(rq_s)
        rd_s[...] = jnp.zeros_like(rd_s)
        dkv_s[...] = jnp.zeros_like(dkv_s) if upper else refs[7][...]

    q = load_queries(n_blk, pos, q_own, q_other)
    do = do_ref[...]
    q_t = q.T
    do_t = do.T
    for h in range(groups):
        rows = slice(h * dim, (h + 1) * dim)
        rq_s[h, :dim, :] = q_t[rows, :]
        rd_s[h, dim:, :] = do_t[rows, :]
        dot_s[h] = jnp.sum(do_t[rows, :].astype(F32) * o_ref[rows, :].astype(F32), axis=0, keepdims=True)
    dqt_s[...] = jnp.zeros_like(dqt_s)

    def tile(j, diag):
        kv_j = kv_s[j]
        k_t = kvt_s[j, :dim, :]
        dk = dkv_s[j, :dim, :]
        dv = dkv_s[j, dim:, :]
        chains = [(h, slice(c, c + BWD_SPLIT)) for h in range(groups) for c in range(0, blk, BWD_SPLIT)]

        def scores(h, cs):
            return (jnp.dot(kv_j, rq_s[h, :, cs], preferred_element_type=F32),
                    jnp.dot(kv_j, rd_s[h, :, cs], preferred_element_type=F32))

        def outputs(dk, dv, h, cs, p, ds):
            dqt_s[h, :, cs] += jnp.dot(k_t, ds, preferred_element_type=F32)
            dk += lax.dot_general(rq_s[h, :dim, cs], ds, NT, preferred_element_type=F32)
            dv += lax.dot_general(rd_s[h, dim:, cs], p, NT, preferred_element_type=F32)
            return dk, dv

        ahead = [scores(*chain) for chain in chains[:BWD_AHEAD]]
        behind = []
        for i, (h, cs) in enumerate(chains):
            if i + BWD_AHEAD < len(chains):
                ahead.append(scores(*chains[i + BWD_AHEAD]))
            s, dp = ahead[i]
            p = jnp.exp(s - lse_ref[h:h + 1, cs])
            if diag:
                p = jnp.where(keep_mask(s.shape, cs.start), p, 0.0)
            ds = (p * (dp - dot_s[h, :, cs])).astype(BF16)
            behind.append((h, cs, p.astype(BF16), ds))
            if len(behind) > BWD_BEHIND:
                dk, dv = outputs(dk, dv, *behind.pop(0))
        for item in behind:
            dk, dv = outputs(dk, dv, *item)
        dkv_s[j, :dim, :] = dk
        dkv_s[j, dim:, :] = dv

    tile(pos, True)

    @pl.loop(0, pos)
    def _(j):
        tile(j, False)

    shard = shard_of(pos, n_blk)
    for h in range(groups):
        g_ref[shard, h * dim:(h + 1) * dim, :] = dqt_s[h].astype(BF16)

    @pl.when(step == count - 1)
    def _():
        for b in range(first, first + count):
            s = b if b < n_blk // 2 else n_blk - 1 - b
            g_ref[s, cols:, :] = dkv_s[b].astype(BF16)
        if upper:
            refs[8][...] = dkv_s[:first]


def key_specs(n_half, blk, groups, dim, first):
    cols = groups * dim
    query = pl.BlockSpec((None, blk, cols), lambda i: (shard_of(first + i, 2 * n_half), 0, 0))
    keys = pl.BlockSpec((n_half, blk, 2 * dim), lambda i: (0, 0, cols // (2 * dim)))
    return [query, query, keys, keys]


def feature_spec(n_blk, cols, blk, first):
    return pl.BlockSpec((None, cols, blk), lambda i: (shard_of(first + i, n_blk), 0, half_of(first + i, n_blk)))


def attend(own, other, prev, first, count, groups, dim):
    n_half, blk = own.shape[:2]
    n_blk = 2 * n_half
    cols = groups * dim
    elems = blk * blk * groups * sum(range(first + 1, first + count + 1))
    out_shape = [jax.ShapeDtypeStruct((n_half, cols, 2 * blk), BF16), jax.ShapeDtypeStruct((n_blk, groups, blk), F32)]
    return pl.pallas_call(
        lambda *refs: fwd_kernel(n_blk, groups, dim, first, *refs),
        grid=(count,),
        in_specs=key_specs(n_half, blk, groups, dim, first) + [pl.BlockSpec(memory_space=pl.ANY)] * len(prev),
        out_specs=[feature_spec(n_blk, cols, blk, first), pl.BlockSpec((None, groups, blk), lambda i: (first + i, 0, 0))],
        out_shape=out_shape,
        input_output_aliases={4 + i: i for i in range(len(prev))},
        scratch_shapes=[
            pltpu.VMEM((n_blk, blk, 2 * dim), BF16),
            pltpu.VMEM((n_blk, 2 * dim, blk), BF16),
            pltpu.VMEM((groups, 2 * dim, blk), BF16),
            pltpu.VMEM((groups, dim, blk), F32),
            pltpu.VMEM((groups, 1, blk), F32),
            pltpu.VMEM((groups, 1, blk), F32),
        ],
        compiler_params=pltpu.CompilerParams(dimension_semantics=("arbitrary",), vmem_limit_bytes=VMEM_LIMIT),
        cost_estimate=pl.CostEstimate(flops=elems * 4 * 4 * dim, bytes_accessed=count * blk * cols * 4, transcendentals=elems),
        name="attend_fwd",
    )(own, other, own, other, *prev)


def attend_grad(own, other, do, o, lse, carried, first, count, groups, dim):
    n_half, blk = own.shape[:2]
    n_blk = 2 * n_half
    cols = groups * dim
    elems = blk * blk * groups * sum(range(first + 1, first + count + 1))
    feats = cols + 2 * dim
    keys_shape = (n_blk if first else n_half, 2 * dim, blk)
    whole = pl.BlockSpec((n_half, 2 * dim, blk), lambda i: (0, 0, 0))
    out_specs = [pl.BlockSpec((n_half, feats, blk), lambda i: (0, 0, 0))] + [whole] * (first > 0)
    out_shape = [jax.ShapeDtypeStruct((n_half, feats, blk), BF16)] + [jax.ShapeDtypeStruct((n_half, 2 * dim, blk), F32)] * (first > 0)
    return pl.pallas_call(
        lambda *refs: bwd_kernel(n_blk, groups, dim, first, count, *refs),
        grid=(count,),
        in_specs=key_specs(n_half, blk, groups, dim, first) + [
            pl.BlockSpec((None, blk, cols), lambda i: (stored_block(first + i, n_blk), 0, 0)),
            feature_spec(n_blk, cols, blk, first),
            pl.BlockSpec((None, groups, blk), lambda i: (first + i, 0, 0))] + [whole] * len(carried),
        out_specs=out_specs,
        out_shape=out_shape,
        scratch_shapes=[
            pltpu.VMEM((n_blk, blk, 2 * dim), BF16),
            pltpu.VMEM((n_blk, 2 * dim, blk), BF16),
            pltpu.VMEM((groups, 2 * dim, blk), BF16),
            pltpu.VMEM((groups, 2 * dim, blk), BF16),
            pltpu.VMEM((groups, 1, blk), F32),
            pltpu.VMEM((groups, dim, blk), F32),
            pltpu.VMEM(keys_shape, F32),
        ],
        compiler_params=pltpu.CompilerParams(dimension_semantics=("arbitrary",), vmem_limit_bytes=VMEM_LIMIT),
        cost_estimate=pl.CostEstimate(flops=elems * 10 * 4 * dim, bytes_accessed=count * blk * cols * 8, transcendentals=elems),
        name="attend_bwd",
    )(own, other, own, other, do, o, lse, *carried)


def solution(mesh):
    seq_shards = mesh.shape["cp"]
    swap = [(0, 1), (1, 0)]

    def device_fn(x_blk, w_query, w_key, w_value, w_out, dy_blk):
        model_dim, q_heads, dim = w_query.shape
        half_rows = x_blk.shape[0]
        kv_heads = w_key.shape[1]
        groups = q_heads // kv_heads
        cols = groups * dim
        feats = cols + 2 * dim
        q_cols = q_heads * dim
        n_half = seq_shards
        n_blk = 2 * seq_shards
        scale = dim ** -0.5
        mine = lax.axis_index("tp")
        quarter = lax.axis_index("cp")
        wo = w_out.reshape(q_cols, model_dim)
        w_all = jnp.concatenate([(w_query * scale).astype(BF16).transpose(1, 2, 0).reshape(kv_heads, cols, model_dim),
                                 w_key.transpose(1, 2, 0), w_value.transpose(1, 2, 0)], axis=1)
        w_flat = w_all.reshape(kv_heads * feats, model_dim)

        def mm(a, b, dims):
            return lax.dot_general(a, b, dims, preferred_element_type=F32)

        def exchange(a):
            return lax.ppermute(a, "tp", swap)

        def switch(a):
            return lax.all_to_all(a, "cp", split_axis=0, concat_axis=0, tiled=True)

        def project(rows):
            return mm(rows, w_flat, NT).astype(BF16).reshape(half_rows, kv_heads, feats).transpose(1, 0, 2)

        def after(value, other):
            return lax.optimization_barrier((value, other))

        def quarter_of(w):
            part = w.shape[0] // seq_shards
            return exchange(lax.dynamic_slice_in_dim(w, quarter * part, part, axis=0))

        def spread(w):
            return lax.all_gather(w, "cp", axis=0, tiled=True)

        x_peer = exchange(x_blk)
        own = switch(project(x_blk))
        x_peer, own = after(x_peer, own)
        dy_late, x_peer = after(dy_blk, x_peer)
        dy_rows = lax.all_gather(dy_late, "tp", axis=0, tiled=True)
        other = switch(project(x_peer))

        partial = attend(own, other, (), 0, n_half, groups, dim)
        dy_ready, partial = after(dy_rows, partial)
        do_own = mm(dy_ready, wo, NT).astype(BF16).reshape(2 * half_rows, kv_heads, cols).transpose(1, 0, 2)
        late, do_own = after((w_flat, wo), do_own)
        do_all = switch(do_own).reshape(n_blk, half_rows, cols)
        quarters = tuple(quarter_of(w) for w in late)
        o_all, lse = attend(own, other, partial, n_half, n_half, groups, dim)
        quarters, o_all = after(quarters, o_all)
        w_peer, wo_peer = (spread(w) for w in quarters)

        o_own = switch(o_all).reshape(q_cols, 2 * half_rows)
        g_upper, carried = attend_grad(own, other, do_all, o_all, lse, (), n_half, n_half, groups, dim)
        g_upper, o_own = after(g_upper, o_own)
        o_mine = lax.dynamic_slice_in_dim(o_own, mine * half_rows, half_rows, axis=1)
        o_peer = exchange(lax.dynamic_slice_in_dim(o_own, (1 - mine) * half_rows, half_rows, axis=1))
        g_upper = switch(g_upper)
        g_lower, = attend_grad(own, other, do_all, o_all, lse, (carried,), 0, n_half, groups, dim)
        g_lower = switch(g_lower)

        is_first = mine == 0
        g_mine = jnp.where(is_first, g_lower, g_upper)
        g_other = jnp.where(is_first, g_upper, g_lower)
        g_peer = exchange(g_other).reshape(kv_heads * feats, half_rows)

        def weight_grad(lo, hi, factor):
            def part(g, rows):
                return mm(g[:, lo:hi].reshape(kv_heads * (hi - lo), half_rows), rows, NN)

            total = part(g_mine, x_blk) + part(g_other, x_peer)
            return (total * factor).astype(BF16).reshape(1, -1, dim, model_dim).transpose(0, 3, 1, 2)

        grad_wo = mm(o_own, dy_rows, NN).astype(BF16).reshape(1, q_heads, dim, model_dim)
        y_blk = (mm(o_mine, wo, TN) + mm(o_peer, wo_peer, TN)).astype(BF16)
        grad_wq = weight_grad(0, cols, scale)
        grad_wk = weight_grad(cols, cols + dim, 1.0)
        grad_wv = weight_grad(cols + dim, feats, 1.0)
        dx_blk = (mm(g_mine.reshape(kv_heads * feats, half_rows), w_flat, TN) + mm(g_peer, w_peer, TN)).astype(BF16)
        return y_blk, dx_blk, grad_wq, grad_wk, grad_wv, grad_wo

    return jax.shard_map(device_fn, mesh=mesh,
                         in_specs=(ROW_SPEC, HEAD_SPEC, HEAD_SPEC, HEAD_SPEC, OUT_W_SPEC, ROW_SPEC),
                         out_specs=(ROW_SPEC, ROW_SPEC, GRAD_SPEC, GRAD_SPEC, GRAD_SPEC, GRAD_OUT_SPEC),
                         check_vma=False)
```

```python
import jax
import jax.numpy as jnp
from jax import lax
from jax.experimental import pallas as pl
from jax.experimental.pallas import tpu as pltpu
from jax.sharding import PartitionSpec as P

ROW_SPEC = P(("dp", "cp", "tp"), None)
HEAD_SPEC = P(None, "tp", None)
OUT_W_SPEC = P("tp", None, None)
GRAD_SPEC = P(("dp", "cp"), None, "tp", None)
GRAD_OUT_SPEC = P(("dp", "cp"), "tp", None, None)
NT = (((1,), (1,)), ((), ()))
NN = (((1,), (0,)), ((), ()))
F32 = jnp.float32
BF16 = jnp.bfloat16
VMEM_LIMIT = 60 * 1024 * 1024
DENSE_LIMIT = 40 * 1024 * 1024
DENSE_TILES = 4
FWD_SPLIT, FWD_AHEAD, FWD_BEHIND = 256, 2, 1
BWD_SPLIT, BWD_AHEAD, BWD_BEHIND = 256, 1, 0


def half_of(pos_blk, n_blk):
    return jnp.where(pos_blk < n_blk // 2, 0, 1)


def shard_of(pos_blk, n_blk):
    return jnp.where(pos_blk < n_blk // 2, pos_blk, n_blk - 1 - pos_blk)


def stored_block(pos_blk, n_blk):
    return 2 * shard_of(pos_blk, n_blk) + half_of(pos_blk, n_blk)


def keep_mask(shape, col=0):
    return lax.broadcasted_iota(jnp.int32, shape, 0) <= lax.broadcasted_iota(jnp.int32, shape, 1) + col


def load_keys(n_blk, own_ref, other_ref, kv_s, kvt_s):
    own_half = lax.axis_index("tp")
    for b in range(n_blk):
        half, shard = (0, b) if b < n_blk // 2 else (1, n_blk - 1 - b)
        block = jnp.where(own_half == half, own_ref[shard], other_ref[shard])
        kv_s[b] = block
        kvt_s[b] = block.T


def load_queries(n_blk, pos, own_ref, other_ref):
    return jnp.where(lax.axis_index("tp") == half_of(pos, n_blk), own_ref[...], other_ref[...])


def fwd_kernel(n_blk, groups, dim, first, *refs):
    q_own, q_other, kv_own, kv_other = refs[:4]
    o_ref, lse_ref, kv_s, kvt_s, rq_s, acc_s, m_s, l_s = refs[-8:]
    pos = first + pl.program_id(0)
    blk = q_own.shape[0]

    @pl.when(pl.program_id(0) == 0)
    def _():
        load_keys(n_blk, kv_own, kv_other, kv_s, kvt_s)
        rq_s[...] = jnp.zeros_like(rq_s)

    q_t = load_queries(n_blk, pos, q_own, q_other).T
    for h in range(groups):
        rq_s[h, :dim, :] = q_t[h * dim:(h + 1) * dim, :]

    def tile(j, diag):
        kv_j = kv_s[j]
        v_t = kvt_s[j, dim:, :]
        chains = [(h, slice(c, c + FWD_SPLIT)) for h in range(groups) for c in range(0, blk, FWD_SPLIT)]

        def scores(h, cs):
            return jnp.dot(kv_j, rq_s[h, :, cs], preferred_element_type=F32)

        def output(h, cs, p, alpha):
            o = jnp.dot(v_t, p, preferred_element_type=F32)
            acc_s[h, :, cs] = o if alpha is None else acc_s[h, :, cs] * alpha + o

        ahead = [scores(*chain) for chain in chains[:FWD_AHEAD]]
        behind = []
        for i, (h, cs) in enumerate(chains):
            if i + FWD_AHEAD < len(chains):
                ahead.append(scores(*chains[i + FWD_AHEAD]))
            s = ahead[i]
            if diag:
                s = jnp.where(keep_mask(s.shape, cs.start), s, -jnp.inf)
                m_new = jnp.max(s, axis=0, keepdims=True)
                p = jnp.exp(s - m_new)
                alpha = None
                l_s[h, :, cs] = jnp.sum(p, axis=0, keepdims=True)
            else:
                m_old = m_s[h, :, cs]
                m_new = jnp.maximum(m_old, jnp.max(s, axis=0, keepdims=True))
                p = jnp.exp(s - m_new)
                alpha = jnp.exp(m_old - m_new)
                l_s[h, :, cs] = l_s[h, :, cs] * alpha + jnp.sum(p, axis=0, keepdims=True)
            m_s[h, :, cs] = m_new
            behind.append((h, cs, p.astype(BF16), alpha))
            if len(behind) > FWD_BEHIND:
                output(*behind.pop(0))
        for item in behind:
            output(*item)

    tile(pos, True)

    @pl.loop(0, pos)
    def _(j):
        tile(j, False)

    for h in range(groups):
        o_ref[h * dim:(h + 1) * dim, :] = (acc_s[h] / l_s[h]).astype(BF16)
        lse_ref[h:h + 1, :] = m_s[h] + jnp.log(l_s[h])


def bwd_kernel(n_blk, groups, dim, first, count, *refs):
    q_own, q_other, kv_own, kv_other, do_ref, o_ref, lse_ref = refs[:7]
    upper = first > 0
    g_ref = refs[7 if upper else 9]
    kv_s, kvt_s, rq_s, rd_s, rdo_s, dot_s, dqt_s, dk_s, dv_s = refs[-9:]
    step = pl.program_id(0)
    pos = first + step
    blk = do_ref.shape[0]
    cols = groups * dim

    @pl.when(step == 0)
    def _():
        load_keys(n_blk, kv_own, kv_other, kv_s, kvt_s)
        rq_s[...] = jnp.zeros_like(rq_s)
        rd_s[...] = jnp.zeros_like(rd_s)
        dk_s[...] = jnp.zeros_like(dk_s) if upper else refs[7][...]
        dv_s[...] = jnp.zeros_like(dv_s) if upper else refs[8][...]

    q = load_queries(n_blk, pos, q_own, q_other)
    do = do_ref[...]
    q_t = q.T
    do_t = do.T
    for h in range(groups):
        rows = slice(h * dim, (h + 1) * dim)
        rq_s[h, :dim, :] = q_t[rows, :]
        rd_s[h, dim:, :] = do_t[rows, :]
        rdo_s[h] = do[:, rows]
        dot_s[h] = jnp.sum(do_t[rows, :].astype(F32) * o_ref[rows, :].astype(F32), axis=0, keepdims=True)
    dqt_s[...] = jnp.zeros_like(dqt_s)

    def tile(j, diag):
        kv_j = kv_s[j]
        k_t = kvt_s[j, :dim, :]
        dk = dk_s[j]
        dv = dv_s[j]
        chains = [(h, slice(c, c + BWD_SPLIT)) for h in range(groups) for c in range(0, blk, BWD_SPLIT)]

        def scores(h, cs):
            return (jnp.dot(kv_j, rq_s[h, :, cs], preferred_element_type=F32),
                    jnp.dot(kv_j, rd_s[h, :, cs], preferred_element_type=F32))

        def outputs(dk, dv, h, cs, p, ds):
            dqt_s[h, :, cs] += jnp.dot(k_t, ds, preferred_element_type=F32)
            dk += lax.dot_general(rq_s[h, :dim, cs], ds, NT, preferred_element_type=F32)
            dv += jnp.dot(p, rdo_s[h, cs, :], preferred_element_type=F32)
            return dk, dv

        ahead = [scores(*chain) for chain in chains[:BWD_AHEAD]]
        behind = []
        for i, (h, cs) in enumerate(chains):
            if i + BWD_AHEAD < len(chains):
                ahead.append(scores(*chains[i + BWD_AHEAD]))
            s, dp = ahead[i]
            p = jnp.exp(s - lse_ref[h:h + 1, cs])
            if diag:
                p = jnp.where(keep_mask(s.shape, cs.start), p, 0.0)
            ds = (p * (dp - dot_s[h, :, cs])).astype(BF16)
            behind.append((h, cs, p.astype(BF16), ds))
            if len(behind) > BWD_BEHIND:
                dk, dv = outputs(dk, dv, *behind.pop(0))
        for item in behind:
            dk, dv = outputs(dk, dv, *item)
        dk_s[j] = dk
        dv_s[j] = dv

    tile(pos, True)

    @pl.loop(0, pos)
    def _(j):
        tile(j, False)

    shard = shard_of(pos, n_blk)
    for h in range(groups):
        g_ref[shard, h * dim:(h + 1) * dim, :] = dqt_s[h].astype(BF16)

    @pl.when(step == count - 1)
    def _():
        for b in range(first, first + count):
            s = b if b < n_blk // 2 else n_blk - 1 - b
            g_ref[s, cols:cols + dim, :] = dk_s[b].astype(BF16)
            g_ref[s, cols + dim:, :] = dv_s[b].T.astype(BF16)
        if upper:
            refs[8][...] = dk_s[:first]
            refs[9][...] = dv_s[:first]


def key_specs(n_half, blk, groups, dim, first):
    cols = groups * dim
    query = pl.BlockSpec((None, blk, cols), lambda i: (shard_of(first + i, 2 * n_half), 0, 0))
    keys = pl.BlockSpec((n_half, blk, 2 * dim), lambda i: (0, 0, cols // (2 * dim)))
    return [query, query, keys, keys]


def feature_spec(n_blk, cols, blk, first):
    return pl.BlockSpec((None, cols, blk), lambda i: (shard_of(first + i, n_blk), 0, half_of(first + i, n_blk)))


def attend(own, other, prev, first, count, groups, dim):
    n_half, blk = own.shape[:2]
    n_blk = 2 * n_half
    cols = groups * dim
    elems = blk * blk * groups * sum(range(first + 1, first + count + 1))
    out_shape = [jax.ShapeDtypeStruct((n_half, cols, 2 * blk), BF16), jax.ShapeDtypeStruct((n_blk, groups, blk), F32)]
    return pl.pallas_call(
        lambda *refs: fwd_kernel(n_blk, groups, dim, first, *refs),
        grid=(count,),
        in_specs=key_specs(n_half, blk, groups, dim, first) + [pl.BlockSpec(memory_space=pl.ANY)] * len(prev),
        out_specs=[feature_spec(n_blk, cols, blk, first), pl.BlockSpec((None, groups, blk), lambda i: (first + i, 0, 0))],
        out_shape=out_shape,
        input_output_aliases={4 + i: i for i in range(len(prev))},
        scratch_shapes=[
            pltpu.VMEM((n_blk, blk, 2 * dim), BF16),
            pltpu.VMEM((n_blk, 2 * dim, blk), BF16),
            pltpu.VMEM((groups, 2 * dim, blk), BF16),
            pltpu.VMEM((groups, dim, blk), F32),
            pltpu.VMEM((groups, 1, blk), F32),
            pltpu.VMEM((groups, 1, blk), F32),
        ],
        compiler_params=pltpu.CompilerParams(dimension_semantics=("arbitrary",), vmem_limit_bytes=VMEM_LIMIT),
        cost_estimate=pl.CostEstimate(flops=elems * 4 * 4 * dim, bytes_accessed=count * blk * cols * 4, transcendentals=elems),
        name="attend_fwd",
    )(own, other, own, other, *prev)


def attend_grad(own, other, do, o, lse, carried, first, count, groups, dim):
    n_half, blk = own.shape[:2]
    n_blk = 2 * n_half
    cols = groups * dim
    elems = blk * blk * groups * sum(range(first + 1, first + count + 1))
    feats = cols + 2 * dim
    held = n_blk if first else n_half
    carry_shapes = [(n_half, dim, blk), (n_half, blk, dim)]
    whole = [pl.BlockSpec(shape, lambda i: (0, 0, 0)) for shape in carry_shapes]
    out_specs = [pl.BlockSpec((n_half, feats, blk), lambda i: (0, 0, 0))] + whole * (first > 0)
    out_shape = [jax.ShapeDtypeStruct((n_half, feats, blk), BF16)] + [
        jax.ShapeDtypeStruct(shape, F32) for shape in carry_shapes] * (first > 0)
    return pl.pallas_call(
        lambda *refs: bwd_kernel(n_blk, groups, dim, first, count, *refs),
        grid=(count,),
        in_specs=key_specs(n_half, blk, groups, dim, first) + [
            pl.BlockSpec((None, blk, cols), lambda i: (stored_block(first + i, n_blk), 0, 0)),
            feature_spec(n_blk, cols, blk, first),
            pl.BlockSpec((None, groups, blk), lambda i: (first + i, 0, 0))] + whole * (len(carried) > 0),
        out_specs=out_specs,
        out_shape=out_shape,
        scratch_shapes=[
            pltpu.VMEM((n_blk, blk, 2 * dim), BF16),
            pltpu.VMEM((n_blk, 2 * dim, blk), BF16),
            pltpu.VMEM((groups, 2 * dim, blk), BF16),
            pltpu.VMEM((groups, 2 * dim, blk), BF16),
            pltpu.VMEM((groups, blk, dim), BF16),
            pltpu.VMEM((groups, 1, blk), F32),
            pltpu.VMEM((groups, dim, blk), F32),
            pltpu.VMEM((held, dim, blk), F32),
            pltpu.VMEM((held, blk, dim), F32),
        ],
        compiler_params=pltpu.CompilerParams(dimension_semantics=("arbitrary",), vmem_limit_bytes=VMEM_LIMIT),
        cost_estimate=pl.CostEstimate(flops=elems * 10 * 4 * dim, bytes_accessed=count * blk * cols * 8, transcendentals=elems),
        name="attend_bwd",
    )(own, other, own, other, do, o, lse, *carried)


def dense_call(kernel, grid, in_specs, out_specs, out_shape, scratch, flops, args):
    return pl.pallas_call(
        kernel, grid=(grid,), in_specs=in_specs, out_specs=out_specs, out_shape=out_shape, scratch_shapes=scratch,
        compiler_params=pltpu.CompilerParams(dimension_semantics=("arbitrary",), vmem_limit_bytes=DENSE_LIMIT),
        cost_estimate=pl.CostEstimate(flops=flops, bytes_accessed=sum(a.size * 2 for a in args), transcendentals=0),
    )(*args)


def project(rows, weight, parts):
    count, depth = rows.shape
    width = weight.shape[0] // parts

    def kernel(a_ref, w_ref, o_ref):
        o_ref[...] = lax.dot_general(a_ref[...], w_ref[...], NT, preferred_element_type=F32).astype(BF16)

    return dense_call(kernel, parts,
                      [pl.BlockSpec((count, depth), lambda i: (0, 0)), pl.BlockSpec((width, depth), lambda i: (i, 0))],
                      pl.BlockSpec((None, count, width), lambda i: (i, 0, 0)),
                      jax.ShapeDtypeStruct((parts, count, width), BF16), [], 2 * count * depth * width * parts, (rows, weight))


def combine(own, w, peer, w_peer, tiles):
    depth = w.shape[0]
    count = own[0].shape[2]
    cols = w.shape[1] // tiles
    pieces = (*own, *peer)

    def kernel(*refs):
        w_ref, wp_ref, o_ref, at_s = refs[-4:]

        @pl.when(pl.program_id(0) == 0)
        def _():
            for base, group in ((0, refs[:len(own)]), (depth, refs[len(own):len(pieces)])):
                width = sum(ref.shape[1] for ref in group)
                for ref in group:
                    for c in range(ref.shape[0]):
                        at_s[:, base + c * width:base + c * width + ref.shape[1]] = ref[c].T
                    base += ref.shape[1]

        total = jnp.dot(at_s[:, :depth], w_ref[...], preferred_element_type=F32)
        total += jnp.dot(at_s[:, depth:], wp_ref[...], preferred_element_type=F32)
        o_ref[...] = total.astype(BF16)

    w_spec = pl.BlockSpec((depth, cols), lambda i: (0, i))
    return dense_call(kernel, tiles,
                      [pl.BlockSpec(p.shape, lambda i: (0, 0, 0)) for p in pieces] + [w_spec, w_spec],
                      pl.BlockSpec((count, cols), lambda i: (0, i)),
                      jax.ShapeDtypeStruct((count, w.shape[1]), BF16), [pltpu.VMEM((count, 2 * depth), BF16)],
                      4 * count * depth * w.shape[1], (*pieces, w, w_peer))


def weight_grads(g, x, g_peer, x_peer, cols, dim, scale):
    heads, feats, count = g.shape
    model = x.shape[1]

    def kernel(g_ref, x_ref, gp_ref, xp_ref, q_ref, k_ref, v_ref):
        def part(lo, hi):
            total = jnp.dot(g_ref[lo:hi, :], x_ref[...], preferred_element_type=F32)
            return total + jnp.dot(gp_ref[lo:hi, :], xp_ref[...], preferred_element_type=F32)

        q_ref[...] = (part(0, cols) * scale).astype(BF16)
        both = part(cols, feats).astype(BF16)
        k_ref[...] = both[:dim]
        v_ref[...] = both[dim:]

    g_spec = pl.BlockSpec((None, feats, count), lambda i: (i, 0, 0))
    x_spec = pl.BlockSpec((count, model), lambda i: (0, 0))
    sizes = (cols, dim, dim)
    return dense_call(kernel, heads, [g_spec, x_spec, g_spec, x_spec],
                      [pl.BlockSpec((n, model), lambda i: (i, 0)) for n in sizes],
                      [jax.ShapeDtypeStruct((heads * n, model), BF16) for n in sizes], [],
                      4 * heads * feats * count * model, (g, x, g_peer, x_peer))


def solution(mesh):
    seq_shards = mesh.shape["cp"]
    swap = [(0, 1), (1, 0)]

    def device_fn(x_blk, w_query, w_key, w_value, w_out, dy_blk):
        model_dim, q_heads, dim = w_query.shape
        half_rows = x_blk.shape[0]
        kv_heads = w_key.shape[1]
        groups = q_heads // kv_heads
        cols = groups * dim
        feats = cols + 2 * dim
        q_cols = q_heads * dim
        n_half = seq_shards
        n_blk = 2 * seq_shards
        scale = dim ** -0.5
        mine = lax.axis_index("tp")
        quarter = lax.axis_index("cp")
        wo = w_out.reshape(q_cols, model_dim)
        w_all = jnp.concatenate([(w_query * scale).astype(BF16).transpose(1, 2, 0).reshape(kv_heads, cols, model_dim),
                                 w_key.transpose(1, 2, 0), w_value.transpose(1, 2, 0)], axis=1)
        w_flat = w_all.reshape(kv_heads * feats, model_dim)

        def mm(a, b, dims):
            return lax.dot_general(a, b, dims, preferred_element_type=F32)

        def exchange(a):
            return lax.ppermute(a, "tp", swap)

        def switch(a):
            return lax.all_to_all(a, "cp", split_axis=0, concat_axis=0, tiled=True)

        def after(value, other):
            return lax.optimization_barrier((value, other))

        def quarter_of(w):
            part = w.shape[0] // seq_shards
            return exchange(lax.dynamic_slice_in_dim(w, quarter * part, part, axis=0))

        def spread(w):
            return lax.all_gather(w, "cp", axis=0, tiled=True)

        x_peer = exchange(x_blk)
        own = switch(project(x_blk, w_flat, kv_heads))
        x_peer, own = after(x_peer, own)
        dy_late, x_peer = after(dy_blk, x_peer)
        dy_rows = lax.all_gather(dy_late, "tp", axis=0, tiled=True)
        other = switch(project(x_peer, w_flat, kv_heads))

        partial = attend(own, other, (), 0, n_half, groups, dim)
        dy_ready, partial = after(dy_rows, partial)
        do_own = project(dy_ready, wo, kv_heads)
        late, do_own = after((w_flat, wo), do_own)
        do_all = switch(do_own).reshape(n_blk, half_rows, cols)
        w_quarter, wo_quarter = (quarter_of(w) for w in late)
        o_all, lse = attend(own, other, partial, n_half, n_half, groups, dim)
        wo_quarter, o_all = after(wo_quarter, o_all)
        wo_peer = spread(wo_quarter)

        o_own = switch(o_all).reshape(q_cols, 2 * half_rows)
        g_upper, *carried = attend_grad(own, other, do_all, o_all, lse, (), n_half, n_half, groups, dim)
        g_upper, o_own = after(g_upper, o_own)
        w_quarter, g_upper = after(w_quarter, g_upper)
        w_peer = spread(w_quarter)
        o_mine = lax.dynamic_slice_in_dim(o_own, mine * half_rows, half_rows, axis=1)
        o_peer = exchange(lax.dynamic_slice_in_dim(o_own, (1 - mine) * half_rows, half_rows, axis=1))
        raw_upper = g_upper
        g_upper = switch(raw_upper)
        raw_lower, = attend_grad(own, other, do_all, o_all, lse, tuple(carried), 0, n_half, groups, dim)

        is_first = mine == 0
        relay = exchange(jnp.where(is_first, raw_upper[:, :cols], raw_lower[:, :cols]))
        g_lower = switch(raw_lower)
        relay = switch(relay)
        g_mine = jnp.where(is_first, g_lower, g_upper)
        g_other = jnp.where(is_first, g_upper, g_lower)
        g_tail = exchange(g_other[:, cols:])

        def heads_last(g):
            return g.reshape(1, -1, dim, model_dim).transpose(0, 3, 1, 2)

        y_blk = combine([o_mine[None]], wo, [o_peer[None]], wo_peer, DENSE_TILES)
        grad_wo = mm(o_own, dy_rows, NN).astype(BF16).reshape(1, q_heads, dim, model_dim)
        grad_wq, grad_wk, grad_wv = map(heads_last, weight_grads(g_mine, x_blk, g_other, x_peer, cols, dim, scale))
        dx_blk = combine([g_mine], w_flat, [relay, g_tail], w_peer, DENSE_TILES)
        return y_blk, dx_blk, grad_wq, grad_wk, grad_wv, grad_wo

    return jax.shard_map(device_fn, mesh=mesh,
                         in_specs=(ROW_SPEC, HEAD_SPEC, HEAD_SPEC, HEAD_SPEC, OUT_W_SPEC, ROW_SPEC),
                         out_specs=(ROW_SPEC, ROW_SPEC, GRAD_SPEC, GRAD_SPEC, GRAD_SPEC, GRAD_OUT_SPEC),
                         check_vma=False)
```

```python
import jax
import jax.numpy as jnp
from jax import lax
from jax.experimental import pallas as pl
from jax.experimental.pallas import tpu as pltpu
from jax.sharding import PartitionSpec as P

ROW_SPEC = P(("dp", "cp", "tp"), None)
HEAD_SPEC = P(None, "tp", None)
OUT_W_SPEC = P("tp", None, None)
GRAD_SPEC = P(("dp", "cp"), None, "tp", None)
GRAD_OUT_SPEC = P(("dp", "cp"), "tp", None, None)
NT = (((1,), (1,)), ((), ()))
F32 = jnp.float32
BF16 = jnp.bfloat16
VMEM_LIMIT = 60 * 1024 * 1024
DENSE_LIMIT = 62 * 1024 * 1024
DENSE_TILES = 4
FWD_SPLIT, FWD_AHEAD, FWD_BEHIND = 256, 2, 1
BWD_SPLIT, BWD_AHEAD, BWD_BEHIND = 256, 1, 0


def half_of(pos_blk, n_blk):
    return jnp.where(pos_blk < n_blk // 2, 0, 1)


def shard_of(pos_blk, n_blk):
    return jnp.where(pos_blk < n_blk // 2, pos_blk, n_blk - 1 - pos_blk)


def stored_block(pos_blk, n_blk):
    return 2 * shard_of(pos_blk, n_blk) + half_of(pos_blk, n_blk)


def keep_mask(shape, col=0):
    return lax.broadcasted_iota(jnp.int32, shape, 0) <= lax.broadcasted_iota(jnp.int32, shape, 1) + col


def load_keys(n_blk, own_ref, other_ref, kv_s, kvt_s):
    own_half = lax.axis_index("tp")
    for b in range(n_blk):
        half, shard = (0, b) if b < n_blk // 2 else (1, n_blk - 1 - b)
        block = jnp.where(own_half == half, own_ref[shard], other_ref[shard])
        kv_s[b] = block
        kvt_s[b] = block.T


def load_queries(n_blk, pos, own_ref, other_ref):
    return jnp.where(lax.axis_index("tp") == half_of(pos, n_blk), own_ref[...], other_ref[...])


def fwd_kernel(n_blk, groups, dim, first, *refs):
    q_own, q_other, kv_own, kv_other = refs[:4]
    o_ref, lse_ref, kv_s, kvt_s, rq_s, acc_s, m_s, l_s = refs[-8:]
    pos = first + pl.program_id(0)
    blk = q_own.shape[0]

    @pl.when(pl.program_id(0) == 0)
    def _():
        load_keys(n_blk, kv_own, kv_other, kv_s, kvt_s)
        rq_s[...] = jnp.zeros_like(rq_s)

    q_t = load_queries(n_blk, pos, q_own, q_other).T
    for h in range(groups):
        rq_s[h, :dim, :] = q_t[h * dim:(h + 1) * dim, :]

    def tile(j, diag):
        kv_j = kv_s[j]
        v_t = kvt_s[j, dim:, :]
        chains = [(h, slice(c, c + FWD_SPLIT)) for h in range(groups) for c in range(0, blk, FWD_SPLIT)]

        def seen(cs):
            return cs.stop if diag else blk

        def scores(h, cs):
            return jnp.dot(kv_j[:seen(cs)], rq_s[h, :, cs], preferred_element_type=F32)

        def output(h, cs, p, alpha):
            o = jnp.dot(v_t[:, :seen(cs)], p, preferred_element_type=F32)
            acc_s[h, :, cs] = o if alpha is None else acc_s[h, :, cs] * alpha + o

        ahead = [scores(*chain) for chain in chains[:FWD_AHEAD]]
        behind = []
        for i, (h, cs) in enumerate(chains):
            if i + FWD_AHEAD < len(chains):
                ahead.append(scores(*chains[i + FWD_AHEAD]))
            s = ahead[i]
            if diag:
                s = jnp.where(keep_mask(s.shape, cs.start), s, -jnp.inf)
                m_new = jnp.max(s, axis=0, keepdims=True)
                p = jnp.exp(s - m_new)
                alpha = None
                l_s[h, :, cs] = jnp.sum(p, axis=0, keepdims=True)
            else:
                m_old = m_s[h, :, cs]
                m_new = jnp.maximum(m_old, jnp.max(s, axis=0, keepdims=True))
                p = jnp.exp(s - m_new)
                alpha = jnp.exp(m_old - m_new)
                l_s[h, :, cs] = l_s[h, :, cs] * alpha + jnp.sum(p, axis=0, keepdims=True)
            m_s[h, :, cs] = m_new
            behind.append((h, cs, p.astype(BF16), alpha))
            if len(behind) > FWD_BEHIND:
                output(*behind.pop(0))
        for item in behind:
            output(*item)

    tile(pos, True)

    @pl.loop(0, pos)
    def _(j):
        tile(j, False)

    for h in range(groups):
        o_ref[h * dim:(h + 1) * dim, :] = (acc_s[h] / l_s[h]).astype(BF16)
        lse_ref[h:h + 1, :] = m_s[h] + jnp.log(l_s[h])


def bwd_kernel(n_blk, groups, dim, first, count, *refs):
    q_own, q_other, kv_own, kv_other, do_ref, o_ref, lse_ref = refs[:7]
    upper = first > 0
    g_ref = refs[7 if upper else 9]
    kv_s, kvt_s, rq_s, rd_s, rdo_s, dot_s, dqt_s, dk_s, dv_s = refs[-9:]
    step = pl.program_id(0)
    pos = first + step
    blk = do_ref.shape[0]
    cols = groups * dim

    @pl.when(step == 0)
    def _():
        load_keys(n_blk, kv_own, kv_other, kv_s, kvt_s)
        rq_s[...] = jnp.zeros_like(rq_s)
        rd_s[...] = jnp.zeros_like(rd_s)
        dk_s[...] = jnp.zeros_like(dk_s) if upper else refs[7][...]
        dv_s[...] = jnp.zeros_like(dv_s) if upper else refs[8][...]

    q = load_queries(n_blk, pos, q_own, q_other)
    do = do_ref[...]
    q_t = q.T
    do_t = do.T
    for h in range(groups):
        rows = slice(h * dim, (h + 1) * dim)
        rq_s[h, :dim, :] = q_t[rows, :]
        rd_s[h, dim:, :] = do_t[rows, :]
        rdo_s[h] = do[:, rows]
        dot_s[h] = jnp.sum(do_t[rows, :].astype(F32) * o_ref[rows, :].astype(F32), axis=0, keepdims=True)
    dqt_s[...] = jnp.zeros_like(dqt_s)

    def tile(j, diag):
        kv_j = kv_s[j]
        k_t = kvt_s[j, :dim, :]
        dk, dv = (None, None) if diag else (dk_s[j], dv_s[j])
        chains = [(h, slice(c, c + BWD_SPLIT)) for h in range(groups) for c in range(0, blk, BWD_SPLIT)]

        def seen(cs):
            return cs.stop if diag else blk

        def scores(h, cs):
            return (jnp.dot(kv_j[:seen(cs)], rq_s[h, :, cs], preferred_element_type=F32),
                    jnp.dot(kv_j[:seen(cs)], rd_s[h, :, cs], preferred_element_type=F32))

        def outputs(dk, dv, h, cs, p, ds):
            dqt_s[h, :, cs] += jnp.dot(k_t[:, :seen(cs)], ds, preferred_element_type=F32)
            dk_part = lax.dot_general(rq_s[h, :dim, cs], ds, NT, preferred_element_type=F32)
            dv_part = jnp.dot(p, rdo_s[h, cs, :], preferred_element_type=F32)
            if diag:
                dk_s[j, :, :seen(cs)] += dk_part
                dv_s[j, :seen(cs), :] += dv_part
                return dk, dv
            return dk + dk_part, dv + dv_part

        ahead = [scores(*chain) for chain in chains[:BWD_AHEAD]]
        behind = []
        for i, (h, cs) in enumerate(chains):
            if i + BWD_AHEAD < len(chains):
                ahead.append(scores(*chains[i + BWD_AHEAD]))
            s, dp = ahead[i]
            p = jnp.exp(s - lse_ref[h:h + 1, cs])
            if diag:
                p = jnp.where(keep_mask(s.shape, cs.start), p, 0.0)
            ds = (p * (dp - dot_s[h, :, cs])).astype(BF16)
            behind.append((h, cs, p.astype(BF16), ds))
            if len(behind) > BWD_BEHIND:
                dk, dv = outputs(dk, dv, *behind.pop(0))
        for item in behind:
            dk, dv = outputs(dk, dv, *item)
        if not diag:
            dk_s[j] = dk
            dv_s[j] = dv

    tile(pos, True)

    @pl.loop(0, pos)
    def _(j):
        tile(j, False)

    shard = shard_of(pos, n_blk)
    for h in range(groups):
        g_ref[shard, h * dim:(h + 1) * dim, :] = dqt_s[h].astype(BF16)

    @pl.when(step == count - 1)
    def _():
        for b in range(first, first + count):
            s = b if b < n_blk // 2 else n_blk - 1 - b
            g_ref[s, cols:cols + dim, :] = dk_s[b].astype(BF16)
            g_ref[s, cols + dim:, :] = dv_s[b].T.astype(BF16)
        if upper:
            refs[8][...] = dk_s[:first]
            refs[9][...] = dv_s[:first]


def key_specs(n_half, blk, groups, dim, first):
    cols = groups * dim
    query = pl.BlockSpec((None, blk, cols), lambda i: (shard_of(first + i, 2 * n_half), 0, 0))
    keys = pl.BlockSpec((n_half, blk, 2 * dim), lambda i: (0, 0, cols // (2 * dim)))
    return [query, query, keys, keys]


def feature_spec(n_blk, cols, blk, first):
    return pl.BlockSpec((None, cols, blk), lambda i: (shard_of(first + i, n_blk), 0, half_of(first + i, n_blk)))


def attend(own, other, prev, first, count, groups, dim):
    n_half, blk = own.shape[:2]
    n_blk = 2 * n_half
    cols = groups * dim
    elems = blk * blk * groups * sum(range(first + 1, first + count + 1))
    out_shape = [jax.ShapeDtypeStruct((n_half, cols, 2 * blk), BF16), jax.ShapeDtypeStruct((n_blk, groups, blk), F32)]
    return pl.pallas_call(
        lambda *refs: fwd_kernel(n_blk, groups, dim, first, *refs),
        grid=(count,),
        in_specs=key_specs(n_half, blk, groups, dim, first) + [pl.BlockSpec(memory_space=pl.ANY)] * len(prev),
        out_specs=[feature_spec(n_blk, cols, blk, first), pl.BlockSpec((None, groups, blk), lambda i: (first + i, 0, 0))],
        out_shape=out_shape,
        input_output_aliases={4 + i: i for i in range(len(prev))},
        scratch_shapes=[
            pltpu.VMEM((n_blk, blk, 2 * dim), BF16),
            pltpu.VMEM((n_blk, 2 * dim, blk), BF16),
            pltpu.VMEM((groups, 2 * dim, blk), BF16),
            pltpu.VMEM((groups, dim, blk), F32),
            pltpu.VMEM((groups, 1, blk), F32),
            pltpu.VMEM((groups, 1, blk), F32),
        ],
        compiler_params=pltpu.CompilerParams(dimension_semantics=("arbitrary",), vmem_limit_bytes=VMEM_LIMIT),
        cost_estimate=pl.CostEstimate(flops=elems * 4 * 4 * dim, bytes_accessed=count * blk * cols * 4, transcendentals=elems),
        name="attend_fwd",
    )(own, other, own, other, *prev)


def attend_grad(own, other, do, o, lse, carried, first, count, groups, dim):
    n_half, blk = own.shape[:2]
    n_blk = 2 * n_half
    cols = groups * dim
    elems = blk * blk * groups * sum(range(first + 1, first + count + 1))
    feats = cols + 2 * dim
    held = n_blk if first else n_half
    carry_shapes = [(n_half, dim, blk), (n_half, blk, dim)]
    whole = [pl.BlockSpec(shape, lambda i: (0, 0, 0)) for shape in carry_shapes]
    out_specs = [pl.BlockSpec((n_half, feats, blk), lambda i: (0, 0, 0))] + whole * (first > 0)
    out_shape = [jax.ShapeDtypeStruct((n_half, feats, blk), BF16)] + [
        jax.ShapeDtypeStruct(shape, F32) for shape in carry_shapes] * (first > 0)
    return pl.pallas_call(
        lambda *refs: bwd_kernel(n_blk, groups, dim, first, count, *refs),
        grid=(count,),
        in_specs=key_specs(n_half, blk, groups, dim, first) + [
            pl.BlockSpec((None, blk, cols), lambda i: (stored_block(first + i, n_blk), 0, 0)),
            feature_spec(n_blk, cols, blk, first),
            pl.BlockSpec((None, groups, blk), lambda i: (first + i, 0, 0))] + whole * (len(carried) > 0),
        out_specs=out_specs,
        out_shape=out_shape,
        scratch_shapes=[
            pltpu.VMEM((n_blk, blk, 2 * dim), BF16),
            pltpu.VMEM((n_blk, 2 * dim, blk), BF16),
            pltpu.VMEM((groups, 2 * dim, blk), BF16),
            pltpu.VMEM((groups, 2 * dim, blk), BF16),
            pltpu.VMEM((groups, blk, dim), BF16),
            pltpu.VMEM((groups, 1, blk), F32),
            pltpu.VMEM((groups, dim, blk), F32),
            pltpu.VMEM((held, dim, blk), F32),
            pltpu.VMEM((held, blk, dim), F32),
        ],
        compiler_params=pltpu.CompilerParams(dimension_semantics=("arbitrary",), vmem_limit_bytes=VMEM_LIMIT),
        cost_estimate=pl.CostEstimate(flops=elems * 10 * 4 * dim, bytes_accessed=count * blk * cols * 8, transcendentals=elems),
        name="attend_bwd",
    )(own, other, own, other, do, o, lse, *carried)


def dense_call(kernel, grid, in_specs, out_specs, out_shape, scratch, flops, args):
    return pl.pallas_call(
        kernel, grid=(grid,), in_specs=in_specs, out_specs=out_specs, out_shape=out_shape, scratch_shapes=scratch,
        compiler_params=pltpu.CompilerParams(dimension_semantics=("arbitrary",), vmem_limit_bytes=DENSE_LIMIT),
        cost_estimate=pl.CostEstimate(flops=flops, bytes_accessed=sum(a.size * 2 for a in args), transcendentals=0),
    )(*args)


def project(rows, weight, parts):
    count, depth = rows.shape
    width = weight.shape[0] // parts

    def kernel(a_ref, w_ref, o_ref):
        o_ref[...] = lax.dot_general(a_ref[...], w_ref[...], NT, preferred_element_type=F32).astype(BF16)

    return dense_call(kernel, parts,
                      [pl.BlockSpec((count, depth), lambda i: (0, 0)), pl.BlockSpec((width, depth), lambda i: (i, 0))],
                      pl.BlockSpec((None, count, width), lambda i: (i, 0, 0)),
                      jax.ShapeDtypeStruct((parts, count, width), BF16), [], 2 * count * depth * width * parts, (rows, weight))


def product(a, b, tiles):
    count = a.shape[0] // tiles

    def kernel(a_ref, b_ref, o_ref):
        o_ref[...] = jnp.dot(a_ref[...], b_ref[...], preferred_element_type=F32).astype(BF16)

    return dense_call(kernel, tiles,
                      [pl.BlockSpec((count, a.shape[1]), lambda i: (i, 0)), pl.BlockSpec(b.shape, lambda i: (0, 0))],
                      pl.BlockSpec((count, b.shape[1]), lambda i: (i, 0)),
                      jax.ShapeDtypeStruct((a.shape[0], b.shape[1]), BF16), [], 2 * a.size * b.shape[1], (a, b))


def combine(own, w, peer, w_peer, tiles):
    depth = w.shape[0]
    count = own[0].shape[2]
    cols = w.shape[1] // tiles
    pieces = (*own, *peer)

    def kernel(*refs):
        w_ref, wp_ref, o_ref, at_s = refs[-4:]

        @pl.when(pl.program_id(0) == 0)
        def _():
            for base, group in ((0, refs[:len(own)]), (depth, refs[len(own):len(pieces)])):
                width = sum(ref.shape[1] for ref in group)
                for ref in group:
                    for c in range(ref.shape[0]):
                        at_s[:, base + c * width:base + c * width + ref.shape[1]] = ref[c].T
                    base += ref.shape[1]

        total = jnp.dot(at_s[:, :depth], w_ref[...], preferred_element_type=F32)
        total += jnp.dot(at_s[:, depth:], wp_ref[...], preferred_element_type=F32)
        o_ref[...] = total.astype(BF16)

    w_spec = pl.BlockSpec((depth, cols), lambda i: (0, i))
    return dense_call(kernel, tiles,
                      [pl.BlockSpec(p.shape, lambda i: (0, 0, 0)) for p in pieces] + [w_spec, w_spec],
                      pl.BlockSpec((count, cols), lambda i: (0, i)),
                      jax.ShapeDtypeStruct((count, w.shape[1]), BF16), [pltpu.VMEM((count, 2 * depth), BF16)],
                      4 * count * depth * w.shape[1], (*pieces, w, w_peer))


def weight_grads(g, x, g_peer, x_peer, cols, dim, scale):
    heads, feats, count = g.shape
    model = x.shape[1]

    def kernel(g_ref, x_ref, gp_ref, xp_ref, q_ref, k_ref, v_ref):
        def part(lo, hi):
            total = jnp.dot(g_ref[lo:hi, :], x_ref[...], preferred_element_type=F32)
            return total + jnp.dot(gp_ref[lo:hi, :], xp_ref[...], preferred_element_type=F32)

        q_ref[...] = (part(0, cols) * scale).astype(BF16)
        both = part(cols, feats).astype(BF16)
        k_ref[...] = both[:dim]
        v_ref[...] = both[dim:]

    g_spec = pl.BlockSpec((None, feats, count), lambda i: (i, 0, 0))
    x_spec = pl.BlockSpec((count, model), lambda i: (0, 0))
    sizes = (cols, dim, dim)
    return dense_call(kernel, heads, [g_spec, x_spec, g_spec, x_spec],
                      [pl.BlockSpec((n, model), lambda i: (i, 0)) for n in sizes],
                      [jax.ShapeDtypeStruct((heads * n, model), BF16) for n in sizes], [],
                      4 * heads * feats * count * model, (g, x, g_peer, x_peer))


def solution(mesh):
    seq_shards = mesh.shape["cp"]
    swap = [(0, 1), (1, 0)]

    def device_fn(x_blk, w_query, w_key, w_value, w_out, dy_blk):
        model_dim, q_heads, dim = w_query.shape
        half_rows = x_blk.shape[0]
        kv_heads = w_key.shape[1]
        groups = q_heads // kv_heads
        cols = groups * dim
        feats = cols + 2 * dim
        q_cols = q_heads * dim
        n_half = seq_shards
        n_blk = 2 * seq_shards
        scale = dim ** -0.5
        mine = lax.axis_index("tp")
        quarter = lax.axis_index("cp")
        wo = w_out.reshape(q_cols, model_dim)
        w_all = jnp.concatenate([(w_query * scale).astype(BF16).transpose(1, 2, 0).reshape(kv_heads, cols, model_dim),
                                 w_key.transpose(1, 2, 0), w_value.transpose(1, 2, 0)], axis=1)
        w_flat = w_all.reshape(kv_heads * feats, model_dim)

        def exchange(a):
            return lax.ppermute(a, "tp", swap)

        def switch(a):
            return lax.all_to_all(a, "cp", split_axis=0, concat_axis=0, tiled=True)

        def after(value, other):
            return lax.optimization_barrier((value, other))

        def quarter_of(w):
            part = w.shape[0] // seq_shards
            return lax.dynamic_slice_in_dim(w, quarter * part, part, axis=0)

        def spread(w):
            return lax.all_gather(w, "cp", axis=0, tiled=True)

        x_peer = exchange(x_blk)
        own = switch(project(x_blk, w_flat, kv_heads))
        pieces = (quarter_of(w_flat), quarter_of(wo))
        (x_peer, pieces), own = after((x_peer, pieces), own)
        dy_late, x_peer = after(dy_blk, x_peer)
        dy_rows = lax.all_gather(dy_late, "tp", axis=0, tiled=True)
        other = switch(project(x_peer, w_flat, kv_heads))

        partial = attend(own, other, (), 0, n_half, groups, dim)
        dy_rows, pieces = after(dy_rows, pieces)
        wo_quarter, w_quarter = exchange(pieces[1]), exchange(pieces[0])
        dy_ready, partial = after(dy_rows, partial)
        do_own = project(dy_ready, wo, kv_heads)
        do_all = switch(do_own).reshape(n_blk, half_rows, cols)
        o_all, lse = attend(own, other, partial, n_half, n_half, groups, dim)
        (wo_quarter, w_quarter), o_all = after((wo_quarter, w_quarter), o_all)
        wo_peer, w_peer = spread(wo_quarter), spread(w_quarter)

        o_own = switch(o_all).reshape(q_cols, 2 * half_rows)
        g_upper, *carried = attend_grad(own, other, do_all, o_all, lse, (), n_half, n_half, groups, dim)
        g_upper, o_own = after(g_upper, o_own)
        o_mine = lax.dynamic_slice_in_dim(o_own, mine * half_rows, half_rows, axis=1)
        o_peer = exchange(lax.dynamic_slice_in_dim(o_own, (1 - mine) * half_rows, half_rows, axis=1))
        raw_upper = g_upper
        g_upper = switch(raw_upper)
        raw_lower, = attend_grad(own, other, do_all, o_all, lse, tuple(carried), 0, n_half, groups, dim)

        is_first = mine == 0
        relay = exchange(jnp.where(is_first, raw_upper[:, :cols], raw_lower[:, :cols]))
        g_lower = switch(raw_lower)
        relay = switch(relay)
        g_mine = jnp.where(is_first, g_lower, g_upper)
        g_other = jnp.where(is_first, g_upper, g_lower)
        g_tail = exchange(g_other[:, cols:])

        def heads_last(g):
            return g.reshape(1, -1, dim, model_dim).transpose(0, 3, 1, 2)

        y_blk = combine([o_mine[None]], wo, [o_peer[None]], wo_peer, DENSE_TILES)
        grad_wo = product(o_own, dy_rows, DENSE_TILES).reshape(1, q_heads, dim, model_dim)
        grad_wq, grad_wk, grad_wv = map(heads_last, weight_grads(g_mine, x_blk, g_other, x_peer, cols, dim, scale))
        dx_blk = combine([g_mine], w_flat, [relay, g_tail], w_peer, DENSE_TILES)
        return y_blk, dx_blk, grad_wq, grad_wk, grad_wv, grad_wo

    return jax.shard_map(device_fn, mesh=mesh,
                         in_specs=(ROW_SPEC, HEAD_SPEC, HEAD_SPEC, HEAD_SPEC, OUT_W_SPEC, ROW_SPEC),
                         out_specs=(ROW_SPEC, ROW_SPEC, GRAD_SPEC, GRAD_SPEC, GRAD_SPEC, GRAD_OUT_SPEC),
                         check_vma=False)
```

```python
import jax
import jax.numpy as jnp
from jax import lax
from jax.experimental import pallas as pl
from jax.experimental.pallas import tpu as pltpu
from jax.sharding import PartitionSpec as P

ROW_SPEC = P(("dp", "cp", "tp"), None)
HEAD_SPEC = P(None, "tp", None)
OUT_W_SPEC = P("tp", None, None)
GRAD_SPEC = P(("dp", "cp"), None, "tp", None)
GRAD_OUT_SPEC = P(("dp", "cp"), "tp", None, None)
NT = (((1,), (1,)), ((), ()))
F32 = jnp.float32
BF16 = jnp.bfloat16
VMEM_LIMIT = 60 * 1024 * 1024
DENSE_LIMIT = 62 * 1024 * 1024
DENSE_TILES = 4
FWD_CUT = 5
FWD_SPLIT, FWD_AHEAD, FWD_BEHIND = 256, 2, 1
BWD_SPLIT, BWD_AHEAD, BWD_BEHIND = 256, 1, 0


def half_of(pos_blk, n_blk):
    return jnp.where(pos_blk < n_blk // 2, 0, 1)


def shard_of(pos_blk, n_blk):
    return jnp.where(pos_blk < n_blk // 2, pos_blk, n_blk - 1 - pos_blk)


def keep_mask(shape, col=0):
    return lax.broadcasted_iota(jnp.int32, shape, 0) <= lax.broadcasted_iota(jnp.int32, shape, 1) + col


def load_keys(n_blk, own_ref, head_ref, tail_ref, kv_s, kvt_s):
    own_half = lax.axis_index("tp")
    for b in range(n_blk):
        half, shard = (0, b) if b < n_blk // 2 else (1, n_blk - 1 - b)
        other = jnp.concatenate([head_ref[shard], tail_ref[shard]], axis=0)
        block = jnp.where(own_half == half, own_ref[shard], other)
        kv_s[b] = block
        kvt_s[b] = block.T


def load_rows(n_blk, pos, own_ref, *other_refs):
    other = jnp.concatenate([ref[...] for ref in other_refs], axis=0)
    return jnp.where(lax.axis_index("tp") == half_of(pos, n_blk), own_ref[...], other)


def fwd_kernel(n_blk, groups, dim, first, *refs):
    q_refs, key_refs = refs[:3], refs[3:6]
    o_ref, lse_ref, kv_s, kvt_s, rq_s, acc_s, m_s, l_s = refs[-8:]
    pos = first + pl.program_id(0)
    blk = q_refs[0].shape[0]

    @pl.when(pl.program_id(0) == 0)
    def _():
        load_keys(n_blk, *key_refs, kv_s, kvt_s)
        rq_s[...] = jnp.zeros_like(rq_s)

    q_t = load_rows(n_blk, pos, *q_refs).T
    for h in range(groups):
        rq_s[h, :dim, :] = q_t[h * dim:(h + 1) * dim, :]

    def tile(j, diag):
        kv_j = kv_s[j]
        v_t = kvt_s[j, dim:, :]
        chains = [(h, slice(c, c + FWD_SPLIT)) for h in range(groups) for c in range(0, blk, FWD_SPLIT)]

        def seen(cs):
            return cs.stop if diag else blk

        def scores(h, cs):
            return jnp.dot(kv_j[:seen(cs)], rq_s[h, :, cs], preferred_element_type=F32)

        def output(h, cs, p, alpha):
            o = jnp.dot(v_t[:, :seen(cs)], p, preferred_element_type=F32)
            acc_s[h, :, cs] = o if alpha is None else acc_s[h, :, cs] * alpha + o

        ahead = [scores(*chain) for chain in chains[:FWD_AHEAD]]
        behind = []
        for i, (h, cs) in enumerate(chains):
            if i + FWD_AHEAD < len(chains):
                ahead.append(scores(*chains[i + FWD_AHEAD]))
            s = ahead[i]
            if diag:
                s = jnp.where(keep_mask(s.shape, cs.start), s, -jnp.inf)
                m_new = jnp.max(s, axis=0, keepdims=True)
                p = jnp.exp(s - m_new)
                alpha = None
                l_s[h, :, cs] = jnp.sum(p, axis=0, keepdims=True)
            else:
                m_old = m_s[h, :, cs]
                m_new = jnp.maximum(m_old, jnp.max(s, axis=0, keepdims=True))
                p = jnp.exp(s - m_new)
                alpha = jnp.exp(m_old - m_new)
                l_s[h, :, cs] = l_s[h, :, cs] * alpha + jnp.sum(p, axis=0, keepdims=True)
            m_s[h, :, cs] = m_new
            behind.append((h, cs, p.astype(BF16), alpha))
            if len(behind) > FWD_BEHIND:
                output(*behind.pop(0))
        for item in behind:
            output(*item)

    tile(pos, True)

    @pl.loop(0, pos)
    def _(j):
        tile(j, False)

    for h in range(groups):
        o_ref[h * dim:(h + 1) * dim, :] = (acc_s[h] / l_s[h]).astype(BF16)
        lse_ref[h:h + 1, :] = m_s[h] + jnp.log(l_s[h])


def bwd_kernel(n_blk, groups, dim, first, count, *refs):
    q_refs, key_refs, do_refs, (o_ref, lse_ref) = refs[:3], refs[3:6], refs[6:8], refs[8:10]
    upper = first > 0
    g_ref = refs[10 if upper else 12]
    kv_s, kvt_s, rq_s, rd_s, rdo_s, dot_s, dqt_s, dk_s, dv_s = refs[-9:]
    step = pl.program_id(0)
    pos = first + step
    blk = do_refs[0].shape[0]
    cols = groups * dim

    @pl.when(step == 0)
    def _():
        load_keys(n_blk, *key_refs, kv_s, kvt_s)
        rq_s[...] = jnp.zeros_like(rq_s)
        rd_s[...] = jnp.zeros_like(rd_s)
        dk_s[...] = jnp.zeros_like(dk_s) if upper else refs[10][...]
        dv_s[...] = jnp.zeros_like(dv_s) if upper else refs[11][...]

    q = load_rows(n_blk, pos, *q_refs)
    do = load_rows(n_blk, pos, *do_refs)
    q_t = q.T
    do_t = do.T
    for h in range(groups):
        rows = slice(h * dim, (h + 1) * dim)
        rq_s[h, :dim, :] = q_t[rows, :]
        rd_s[h, dim:, :] = do_t[rows, :]
        rdo_s[h] = do[:, rows]
        dot_s[h] = jnp.sum(do_t[rows, :].astype(F32) * o_ref[rows, :].astype(F32), axis=0, keepdims=True)
    dqt_s[...] = jnp.zeros_like(dqt_s)

    def tile(j, diag):
        kv_j = kv_s[j]
        k_t = kvt_s[j, :dim, :]
        dk, dv = (None, None) if diag else (dk_s[j], dv_s[j])
        chains = [(h, slice(c, c + BWD_SPLIT)) for h in range(groups) for c in range(0, blk, BWD_SPLIT)]

        def seen(cs):
            return cs.stop if diag else blk

        def scores(h, cs):
            return (jnp.dot(kv_j[:seen(cs)], rq_s[h, :, cs], preferred_element_type=F32),
                    jnp.dot(kv_j[:seen(cs)], rd_s[h, :, cs], preferred_element_type=F32))

        def outputs(dk, dv, h, cs, p, ds):
            dqt_s[h, :, cs] += jnp.dot(k_t[:, :seen(cs)], ds, preferred_element_type=F32)
            dk_part = lax.dot_general(rq_s[h, :dim, cs], ds, NT, preferred_element_type=F32)
            dv_part = jnp.dot(p, rdo_s[h, cs, :], preferred_element_type=F32)
            if diag:
                dk_s[j, :, :seen(cs)] += dk_part
                dv_s[j, :seen(cs), :] += dv_part
                return dk, dv
            return dk + dk_part, dv + dv_part

        ahead = [scores(*chain) for chain in chains[:BWD_AHEAD]]
        behind = []
        for i, (h, cs) in enumerate(chains):
            if i + BWD_AHEAD < len(chains):
                ahead.append(scores(*chains[i + BWD_AHEAD]))
            s, dp = ahead[i]
            p = jnp.exp(s - lse_ref[h:h + 1, cs])
            if diag:
                p = jnp.where(keep_mask(s.shape, cs.start), p, 0.0)
            ds = (p * (dp - dot_s[h, :, cs])).astype(BF16)
            behind.append((h, cs, p.astype(BF16), ds))
            if len(behind) > BWD_BEHIND:
                dk, dv = outputs(dk, dv, *behind.pop(0))
        for item in behind:
            dk, dv = outputs(dk, dv, *item)
        if not diag:
            dk_s[j] = dk
            dv_s[j] = dv

    tile(pos, True)

    @pl.loop(0, pos)
    def _(j):
        tile(j, False)

    shard = shard_of(pos, n_blk)
    for h in range(groups):
        g_ref[shard, h * dim:(h + 1) * dim, :] = dqt_s[h].astype(BF16)

    @pl.when(step == count - 1)
    def _():
        for b in range(first, first + count):
            s = b if b < n_blk // 2 else n_blk - 1 - b
            g_ref[s, cols:cols + dim, :] = dk_s[b].astype(BF16)
            g_ref[s, cols + dim:, :] = dv_s[b].T.astype(BF16)
        if upper:
            refs[11][...] = dk_s[:first]
            refs[12][...] = dv_s[:first]


def key_specs(n_half, blk, groups, dim, first):
    cols = groups * dim
    sizes = (blk, blk // 2, blk // 2)
    queries = [pl.BlockSpec((None, n, cols), lambda i: (shard_of(first + i, 2 * n_half), 0, 0)) for n in sizes]
    keys = [pl.BlockSpec((n_half, n, 2 * dim), lambda i: (0, 0, cols // (2 * dim))) for n in sizes]
    return queries + keys


def feature_spec(n_blk, cols, blk, first):
    return pl.BlockSpec((None, cols, blk), lambda i: (shard_of(first + i, n_blk), 0, half_of(first + i, n_blk)))


def attend(own, other, prev, first, count, groups, dim):
    n_half, blk = own.shape[:2]
    n_blk = 2 * n_half
    cols = groups * dim
    elems = blk * blk * groups * sum(range(first + 1, first + count + 1))
    out_shape = [jax.ShapeDtypeStruct((n_half, cols, 2 * blk), BF16), jax.ShapeDtypeStruct((n_blk, groups, blk), F32)]
    return pl.pallas_call(
        lambda *refs: fwd_kernel(n_blk, groups, dim, first, *refs),
        grid=(count,),
        in_specs=key_specs(n_half, blk, groups, dim, first) + [pl.BlockSpec(memory_space=pl.ANY)] * len(prev),
        out_specs=[feature_spec(n_blk, cols, blk, first), pl.BlockSpec((None, groups, blk), lambda i: (first + i, 0, 0))],
        out_shape=out_shape,
        input_output_aliases={6 + i: i for i in range(len(prev))},
        scratch_shapes=[
            pltpu.VMEM((n_blk, blk, 2 * dim), BF16),
            pltpu.VMEM((n_blk, 2 * dim, blk), BF16),
            pltpu.VMEM((groups, 2 * dim, blk), BF16),
            pltpu.VMEM((groups, dim, blk), F32),
            pltpu.VMEM((groups, 1, blk), F32),
            pltpu.VMEM((groups, 1, blk), F32),
        ],
        compiler_params=pltpu.CompilerParams(dimension_semantics=("arbitrary",), vmem_limit_bytes=VMEM_LIMIT),
        cost_estimate=pl.CostEstimate(flops=elems * 4 * 4 * dim, bytes_accessed=count * blk * cols * 4, transcendentals=elems),
        name="attend_fwd",
    )(own, *other, own, *other, *prev)


def attend_grad(own, other, do, o, lse, carried, first, count, groups, dim):
    n_half, blk = own.shape[:2]
    n_blk = 2 * n_half
    cols = groups * dim
    elems = blk * blk * groups * sum(range(first + 1, first + count + 1))
    feats = cols + 2 * dim
    held = n_blk if first else n_half
    carry_shapes = [(n_half, dim, blk), (n_half, blk, dim)]
    whole = [pl.BlockSpec(shape, lambda i: (0, 0, 0)) for shape in carry_shapes]
    out_specs = [pl.BlockSpec((n_half, feats, blk), lambda i: (0, 0, 0))] + whole * (first > 0)
    out_shape = [jax.ShapeDtypeStruct((n_half, feats, blk), BF16)] + [
        jax.ShapeDtypeStruct(shape, F32) for shape in carry_shapes] * (first > 0)
    return pl.pallas_call(
        lambda *refs: bwd_kernel(n_blk, groups, dim, first, count, *refs),
        grid=(count,),
        in_specs=key_specs(n_half, blk, groups, dim, first) + [
            pl.BlockSpec((None, blk, cols), lambda i: (shard_of(first + i, n_blk), 0, 0)),
            pl.BlockSpec((None, blk, cols), lambda i: (shard_of(first + i, n_blk), 0, 0)),
            feature_spec(n_blk, cols, blk, first),
            pl.BlockSpec((None, groups, blk), lambda i: (first + i, 0, 0))] + whole * (len(carried) > 0),
        out_specs=out_specs,
        out_shape=out_shape,
        scratch_shapes=[
            pltpu.VMEM((n_blk, blk, 2 * dim), BF16),
            pltpu.VMEM((n_blk, 2 * dim, blk), BF16),
            pltpu.VMEM((groups, 2 * dim, blk), BF16),
            pltpu.VMEM((groups, 2 * dim, blk), BF16),
            pltpu.VMEM((groups, blk, dim), BF16),
            pltpu.VMEM((groups, 1, blk), F32),
            pltpu.VMEM((groups, dim, blk), F32),
            pltpu.VMEM((held, dim, blk), F32),
            pltpu.VMEM((held, blk, dim), F32),
        ],
        compiler_params=pltpu.CompilerParams(dimension_semantics=("arbitrary",), vmem_limit_bytes=VMEM_LIMIT),
        cost_estimate=pl.CostEstimate(flops=elems * 10 * 4 * dim, bytes_accessed=count * blk * cols * 8, transcendentals=elems),
        name="attend_bwd",
    )(own, *other, own, *other, *do, o, lse, *carried)


def dense_call(kernel, grid, in_specs, out_specs, out_shape, scratch, flops, args):
    return pl.pallas_call(
        kernel, grid=(grid,), in_specs=in_specs, out_specs=out_specs, out_shape=out_shape, scratch_shapes=scratch,
        compiler_params=pltpu.CompilerParams(dimension_semantics=("arbitrary",), vmem_limit_bytes=DENSE_LIMIT),
        cost_estimate=pl.CostEstimate(flops=flops, bytes_accessed=sum(a.size * 2 for a in args), transcendentals=0),
    )(*args)


def project(rows, weight, parts):
    count, depth = rows.shape
    width = weight.shape[0] // parts

    def kernel(a_ref, w_ref, o_ref):
        o_ref[...] = lax.dot_general(a_ref[...], w_ref[...], NT, preferred_element_type=F32).astype(BF16)

    return dense_call(kernel, parts,
                      [pl.BlockSpec((count, depth), lambda i: (0, 0)), pl.BlockSpec((width, depth), lambda i: (i, 0))],
                      pl.BlockSpec((None, count, width), lambda i: (i, 0, 0)),
                      jax.ShapeDtypeStruct((parts, count, width), BF16), [], 2 * count * depth * width * parts, (rows, weight))


def product(a, b, a_peer, b_peer, tiles):
    count = a.shape[0] // tiles

    def kernel(a_ref, b_ref, ap_ref, bp_ref, o_ref):
        total = jnp.dot(a_ref[...], b_ref[...], preferred_element_type=F32)
        o_ref[...] = (total + jnp.dot(ap_ref[...], bp_ref[...], preferred_element_type=F32)).astype(BF16)

    a_spec = pl.BlockSpec((count, a.shape[1]), lambda i: (i, 0))
    b_spec = pl.BlockSpec(b.shape, lambda i: (0, 0))
    return dense_call(kernel, tiles, [a_spec, b_spec, a_spec, b_spec],
                      pl.BlockSpec((count, b.shape[1]), lambda i: (i, 0)),
                      jax.ShapeDtypeStruct((a.shape[0], b.shape[1]), BF16), [], 4 * a.size * b.shape[1],
                      (a, b, a_peer, b_peer))


def combine(own, w, peer, w_peer, tiles):
    depth = w.shape[0]
    count = own[0].shape[2]
    cols = w.shape[1] // tiles
    pieces = (*own, *peer)

    def kernel(*refs):
        w_ref, wp_ref, o_ref, at_s = refs[-4:]

        @pl.when(pl.program_id(0) == 0)
        def _():
            for base, group in ((0, refs[:len(own)]), (depth, refs[len(own):len(pieces)])):
                width = sum(ref.shape[1] for ref in group)
                for ref in group:
                    for c in range(ref.shape[0]):
                        at_s[:, base + c * width:base + c * width + ref.shape[1]] = ref[c].T
                    base += ref.shape[1]

        total = jnp.dot(at_s[:, :depth], w_ref[...], preferred_element_type=F32)
        total += jnp.dot(at_s[:, depth:], wp_ref[...], preferred_element_type=F32)
        o_ref[...] = total.astype(BF16)

    w_spec = pl.BlockSpec((depth, cols), lambda i: (0, i))
    return dense_call(kernel, tiles,
                      [pl.BlockSpec(p.shape, lambda i: (0, 0, 0)) for p in pieces] + [w_spec, w_spec],
                      pl.BlockSpec((count, cols), lambda i: (0, i)),
                      jax.ShapeDtypeStruct((count, w.shape[1]), BF16), [pltpu.VMEM((count, 2 * depth), BF16)],
                      4 * count * depth * w.shape[1], (*pieces, w, w_peer))


def weight_grads(g, x, g_peer, x_peers, cols, dim, scale):
    heads, feats, count = g.shape
    model = x.shape[1]

    def kernel(g_ref, x_ref, gp_ref, xa_ref, xb_ref, q_ref, k_ref, v_ref):
        def part(lo, hi):
            total = jnp.dot(g_ref[lo:hi, :], x_ref[...], preferred_element_type=F32)
            total += jnp.dot(gp_ref[lo:hi, :count // 2], xa_ref[...], preferred_element_type=F32)
            return total + jnp.dot(gp_ref[lo:hi, count // 2:], xb_ref[...], preferred_element_type=F32)

        q_ref[...] = (part(0, cols) * scale).astype(BF16)
        both = part(cols, feats).astype(BF16)
        k_ref[...] = both[:dim]
        v_ref[...] = both[dim:]

    g_spec = pl.BlockSpec((None, feats, count), lambda i: (i, 0, 0))
    x_spec = pl.BlockSpec((count, model), lambda i: (0, 0))
    half_spec = pl.BlockSpec((count // 2, model), lambda i: (0, 0))
    sizes = (cols, dim, dim)
    return dense_call(kernel, heads, [g_spec, x_spec, g_spec, half_spec, half_spec],
                      [pl.BlockSpec((n, model), lambda i: (i, 0)) for n in sizes],
                      [jax.ShapeDtypeStruct((heads * n, model), BF16) for n in sizes], [],
                      4 * heads * feats * count * model, (g, x, g_peer, *x_peers))


def solution(mesh):
    seq_shards = mesh.shape["cp"]
    swap = [(0, 1), (1, 0)]

    def device_fn(x_blk, w_query, w_key, w_value, w_out, dy_blk):
        model_dim, q_heads, dim = w_query.shape
        half_rows = x_blk.shape[0]
        kv_heads = w_key.shape[1]
        groups = q_heads // kv_heads
        cols = groups * dim
        feats = cols + 2 * dim
        q_cols = q_heads * dim
        n_half = seq_shards
        n_blk = 2 * seq_shards
        scale = dim ** -0.5
        mine = lax.axis_index("tp")
        quarter = lax.axis_index("cp")
        wo = w_out.reshape(q_cols, model_dim)
        w_all = jnp.concatenate([(w_query * scale).astype(BF16).transpose(1, 2, 0).reshape(kv_heads, cols, model_dim),
                                 w_key.transpose(1, 2, 0), w_value.transpose(1, 2, 0)], axis=1)
        w_flat = w_all.reshape(kv_heads * feats, model_dim)

        def exchange(a):
            return lax.ppermute(a, "tp", swap)

        def switch(a):
            return lax.all_to_all(a, "cp", split_axis=0, concat_axis=0, tiled=True)

        def after(value, other):
            return lax.optimization_barrier((value, other))

        def quarter_of(w):
            part = w.shape[0] // seq_shards
            return lax.dynamic_slice_in_dim(w, quarter * part, part, axis=0)

        def spread(w):
            return lax.all_gather(w, "cp", axis=0, tiled=True)

        half = half_rows // 2
        x_head = exchange(x_blk[:half])
        x_tail = exchange(x_blk[half:])
        own = project(x_blk, w_flat, kv_heads)
        x_head, own = after(x_head, own)
        own = switch(own)
        head = project(x_head, w_flat, kv_heads)
        head, own = after(head, own)
        dy_first, head = after(dy_blk, head)
        do_own = project(dy_first, wo, kv_heads)
        head = switch(head)
        pieces = (quarter_of(w_flat), quarter_of(wo))
        x_tail, (do_own, pieces) = after(x_tail, (do_own, pieces))
        dy_late, x_tail = after(dy_blk, x_tail)
        dy_peer = exchange(dy_late)
        tail = project(x_tail, w_flat, kv_heads)
        tail, head = after(tail, head)
        other = (head, switch(tail))
        do_own = switch(after(do_own, other[1])[0])

        partial = attend(own, other, (), 0, FWD_CUT, groups, dim)
        (dy_peer, pieces), partial = after((dy_peer, pieces), partial)
        w_quarter, wo_quarter = exchange(pieces[0]), exchange(pieces[1])
        do_other = project(dy_peer, wo, kv_heads)
        do_other, do_own = after(do_other, do_own)
        do_all = (do_own, switch(do_other))
        o_all, lse = attend(own, other, partial, FWD_CUT, n_blk - FWD_CUT, groups, dim)
        w_quarter, o_all = after(w_quarter, o_all)
        w_peer = spread(w_quarter)

        o_own = switch(o_all).reshape(q_cols, 2 * half_rows)
        g_upper, *carried = attend_grad(own, other, do_all, o_all, lse, (), n_half, n_half, groups, dim)
        g_upper, o_own = after(g_upper, o_own)
        (wo_quarter, w_peer), g_upper = after((wo_quarter, w_peer), g_upper)
        wo_peer = spread(wo_quarter)
        o_mine = lax.dynamic_slice_in_dim(o_own, mine * half_rows, half_rows, axis=1)
        o_other = lax.dynamic_slice_in_dim(o_own, (1 - mine) * half_rows, half_rows, axis=1)
        o_peer = exchange(o_other)
        raw_upper = g_upper
        g_upper = switch(raw_upper)
        raw_lower, = attend_grad(own, other, do_all, o_all, lse, tuple(carried), 0, n_half, groups, dim)

        is_first = mine == 0
        relay = exchange(jnp.where(is_first, raw_upper[:, :cols], raw_lower[:, :cols]))
        g_lower = switch(raw_lower)
        relay = switch(relay)
        g_mine = jnp.where(is_first, g_lower, g_upper)
        g_other = jnp.where(is_first, g_upper, g_lower)
        g_tail = exchange(g_other[:, cols:])

        def heads_last(g):
            return g.reshape(1, -1, dim, model_dim).transpose(0, 3, 1, 2)

        y_blk = combine([o_mine[None]], wo, [o_peer[None]], wo_peer, DENSE_TILES)
        grad_wo = product(o_mine, dy_blk, o_other, dy_peer, DENSE_TILES).reshape(1, q_heads, dim, model_dim)
        grad_wq, grad_wk, grad_wv = map(heads_last, weight_grads(g_mine, x_blk, g_other, (x_head, x_tail), cols, dim, scale))
        dx_blk = combine([g_mine], w_flat, [relay, g_tail], w_peer, DENSE_TILES)
        return y_blk, dx_blk, grad_wq, grad_wk, grad_wv, grad_wo

    return jax.shard_map(device_fn, mesh=mesh,
                         in_specs=(ROW_SPEC, HEAD_SPEC, HEAD_SPEC, HEAD_SPEC, OUT_W_SPEC, ROW_SPEC),
                         out_specs=(ROW_SPEC, ROW_SPEC, GRAD_SPEC, GRAD_SPEC, GRAD_SPEC, GRAD_OUT_SPEC),
                         check_vma=False)
```
